64 devices in a mesh: dp: 4 (over x, y), ep: 16 (over z, core).
Axes of the slice: x: 2, y: 2, z: 8, core: 2. Of those that a mesh axis runs over, the one named last changes fastest.
The devices are a block of a 4x4x8 slice.
Arguments:
- tok_in: bfloat16 [2048, 2048], P(('dp', 'ep')), parts along dimension 0
- lat_cache: bfloat16 [2048, 64, 512], P(('dp', 'ep')), parts along dimension 0
- rope_cache: bfloat16 [2048, 64, 64], P(('dp', 'ep')), parts along dimension 0
- tok_pos: int32 [2048], P(('dp', 'ep')), parts along dimension 0
- expert_ids: int32 [2048, 6], P(('dp', 'ep')), parts along dimension 0
- attn_gain: bfloat16 [2048], replicated
- w_query: bfloat16 [2048, 3072], replicated
- w_kvdown: bfloat16 [2048, 576], replicated
- w_ukey: bfloat16 [16, 128, 512], replicated
- w_uval: bfloat16 [16, 512, 128], replicated
- w_out: bfloat16 [2048, 2048], replicated
- ffn_gain: bfloat16 [2048], replicated
- w_router: bfloat16 [2048, 64], replicated
- sh_gate: bfloat16 [2048, 2816], replicated
- sh_up: bfloat16 [2048, 2816], replicated
- sh_down: bfloat16 [2816, 2048], replicated
- ex_gate: bfloat16 [64, 2048, 1408], P('ep')
- ex_up: bfloat16 [64, 2048, 1408], P('ep')
- ex_down: bfloat16 [64, 1408, 2048], P('ep')
Outputs:
- output 1: bfloat16 [2048, 2048], P(('dp', 'ep')), parts along dimension 0
- output 2: bfloat16 [2048, 64, 512], P(('dp', 'ep')), parts along dimension 0
- output 3: bfloat16 [2048, 64, 64], P(('dp', 'ep')), parts along dimension 0
There are 4 independent parts. The reference program is written for one: setup_inputs(seed, part) draws one part's arguments, and reference() takes and returns one part's arrays. A program takes and returns all parts, laid end to end along the dimension named above; an argument that names none is the same for every part.
All inputs are finite; a program needn't handle non-finite values.
Results may differ from the reference program's by a relative error of at most 0.0130062.
Values are sent between devices in bfloat16 or wider.
A program may use at most 768 MiB of HBM per device.

```python
import jax
import jax.numpy as jnp
from jax import lax

D_MODEL = 2048
EXP_FF = 1408
NUM_EXPERTS = 64
TOP_K = 6
SHARED_FF = 2816
NUM_HEADS = 16
NOPE_DIM = 128
ROPE_DIM = 64
V_DIM = 128
KV_RANK = 512
TOKENS_DEV = 32
SEQ_LEN = 64
EP_SIZE = 16

NUM_TOKENS = EP_SIZE * TOKENS_DEV
QK_DIM = NOPE_DIM + ROPE_DIM
ATTN_SCALE = QK_DIM ** -0.5
ROUTE_SCALE = 2.827
ROPE_BASE = 10000.0
NORM_EPS = 1e-6


def unit_norm(values):
    mean_sq = jnp.mean(jnp.square(values), axis=-1, keepdims=True)
    return values * lax.rsqrt(mean_sq + NORM_EPS)


def rms_norm(values, gain_vec):
    return unit_norm(values) * gain_vec.astype(jnp.float32)


def rope_rotate(values, angle_rad):
    half_dim = values.shape[-1] // 2
    x_first = values[..., :half_dim]
    x_second = values[..., half_dim:]
    cos_part = jnp.cos(angle_rad)
    sin_part = jnp.sin(angle_rad)
    return jnp.concatenate([x_first * cos_part - x_second * sin_part, x_second * cos_part + x_first * sin_part], axis=-1)


def draw_routing(key):
    cap_slots = max(2, -(-2 * TOKENS_DEV * TOP_K // NUM_EXPERTS))
    pick_total = TOKENS_DEV * TOP_K
    hot_count = pick_total // (2 * cap_slots)
    rest_picks = pick_total - hot_count * cap_slots
    cold_count = NUM_EXPERTS - hot_count
    rank_ids = jnp.arange(NUM_EXPERTS)
    extra_one = ((rank_ids >= hot_count) & (rank_ids < hot_count + rest_picks % cold_count)).astype(jnp.int32)
    count_per = jnp.where(rank_ids < hot_count, cap_slots, rest_picks // cold_count + extra_one)
    slot_ends = jnp.cumsum(count_per)
    slot_rank = jnp.sum((jnp.arange(pick_total)[:, None] >= slot_ends[None, :]).astype(jnp.int32), axis=1)
    rank_table = slot_rank.reshape(TOP_K, TOKENS_DEV).T
    key_perm, key_rows, key_pos, key_high, key_low = jax.random.split(key, 5)
    expert_perm = jax.random.permutation(key_perm, NUM_EXPERTS)
    row_perms = jax.vmap(lambda sub_key: jax.random.permutation(sub_key, TOKENS_DEV))(jax.random.split(key_rows, EP_SIZE))
    rank_rows = rank_table[row_perms]
    expert_ids = expert_perm[rank_rows].reshape(NUM_TOKENS, TOP_K).astype(jnp.int32)
    pos_draw = jax.random.randint(key_pos, (NUM_TOKENS,), SEQ_LEN // 4, SEQ_LEN)
    high_slot = jax.random.randint(key_high, (), 0, NUM_TOKENS)
    low_slot = (high_slot + jax.random.randint(key_low, (), 1, NUM_TOKENS)) % NUM_TOKENS
    tok_ids = jnp.arange(NUM_TOKENS)
    tok_pos = jnp.where(tok_ids == high_slot, SEQ_LEN - 1, jnp.where(tok_ids == low_slot, SEQ_LEN // 4, pos_draw)).astype(jnp.int32)
    return expert_ids, tok_pos


def setup_inputs(seed: int = 0, part: int = 0) -> dict:
    base_key = jax.random.key(seed)
    part_keys = jax.random.split(jax.random.fold_in(base_key, part), 4)
    weight_keys = jax.random.split(base_key, 16)
    expert_ids, tok_pos = draw_routing(jax.random.fold_in(part_keys[0], 1))

    def gain_draw(key, size, center):
        return (center + 0.2 * jax.random.normal(key, (size,), jnp.float32)).astype(jnp.bfloat16)

    def weight_draw(key, shape, fan_in, factor):
        return (jax.random.normal(key, shape, jnp.float32) * factor * fan_in ** -0.5).astype(jnp.bfloat16)

    tok_in = jax.random.normal(part_keys[1], (NUM_TOKENS, D_MODEL), jnp.float32).astype(jnp.bfloat16)
    lat_cache = (1.3 * jax.random.normal(part_keys[2], (NUM_TOKENS, SEQ_LEN, KV_RANK), jnp.float32)).astype(jnp.bfloat16)
    rope_cache = jax.random.normal(part_keys[3], (NUM_TOKENS, SEQ_LEN, ROPE_DIM), jnp.float32).astype(jnp.bfloat16)
    return {
        'tok_in': tok_in,
        'lat_cache': lat_cache,
        'rope_cache': rope_cache,
        'tok_pos': tok_pos,
        'expert_ids': expert_ids,
        'attn_gain': gain_draw(weight_keys[0], D_MODEL, 1.0),
        'w_query': weight_draw(weight_keys[1], (D_MODEL, NUM_HEADS * QK_DIM), D_MODEL, 1.0),
        'w_kvdown': weight_draw(weight_keys[2], (D_MODEL, KV_RANK + ROPE_DIM), D_MODEL, 1.0),
        'w_ukey': weight_draw(weight_keys[4], (NUM_HEADS, NOPE_DIM, KV_RANK), NOPE_DIM, 1.0),
        'w_uval': weight_draw(weight_keys[5], (NUM_HEADS, KV_RANK, V_DIM), KV_RANK, 1.0),
        'w_out': weight_draw(weight_keys[6], (NUM_HEADS * V_DIM, D_MODEL), NUM_HEADS * V_DIM, 1.0),
        'ffn_gain': gain_draw(weight_keys[7], D_MODEL, 1.0),
        'w_router': weight_draw(weight_keys[8], (D_MODEL, NUM_EXPERTS), D_MODEL, 2.0),
        'sh_gate': weight_draw(weight_keys[9], (D_MODEL, SHARED_FF), D_MODEL, 1.0),
        'sh_up': weight_draw(weight_keys[10], (D_MODEL, SHARED_FF), D_MODEL, 1.0),
        'sh_down': weight_draw(weight_keys[11], (SHARED_FF, D_MODEL), SHARED_FF, 1.0),
        'ex_gate': weight_draw(weight_keys[12], (NUM_EXPERTS, D_MODEL, EXP_FF), D_MODEL, 1.0),
        'ex_up': weight_draw(weight_keys[13], (NUM_EXPERTS, D_MODEL, EXP_FF), D_MODEL, 1.0),
        'ex_down': weight_draw(weight_keys[14], (NUM_EXPERTS, EXP_FF, D_MODEL), EXP_FF, 1.0),
    }


def reference(tok_in, lat_cache, rope_cache, tok_pos, expert_ids, attn_gain, w_query, w_kvdown, w_ukey, w_uval, w_out, ffn_gain, w_router, sh_gate, sh_up, sh_down, ex_gate, ex_up, ex_down):
    x_wide = tok_in.astype(jnp.float32)
    x_norm = rms_norm(x_wide, attn_gain).astype(jnp.bfloat16)
    q_all = jnp.dot(x_norm, w_query, preferred_element_type=jnp.float32).astype(jnp.bfloat16).reshape(NUM_TOKENS, NUM_HEADS, QK_DIM)
    kv_all = jnp.dot(x_norm, w_kvdown, preferred_element_type=jnp.float32)
    inv_freq = ROPE_BASE ** (-(2.0 * jnp.arange(ROPE_DIM // 2)) / ROPE_DIM)
    angle_rad = tok_pos.astype(jnp.float32)[:, None] * inv_freq[None, :]
    lat_new = unit_norm(kv_all[:, :KV_RANK]).astype(jnp.bfloat16)
    rope_new = rope_rotate(kv_all[:, KV_RANK:], angle_rad).astype(jnp.bfloat16)
    q_rope = rope_rotate(q_all[:, :, NOPE_DIM:].astype(jnp.float32), angle_rad[:, None, :]).astype(jnp.bfloat16)
    q_lat = jnp.einsum('bhn,hnc->bhc', q_all[:, :, :NOPE_DIM].astype(jnp.float32), w_ukey.astype(jnp.float32)).astype(jnp.bfloat16)
    seq_ids = jnp.arange(SEQ_LEN)
    at_pos = (seq_ids[None, :] == tok_pos[:, None])[:, :, None]
    lat_out = jnp.where(at_pos, lat_new[:, None, :], lat_cache)
    rope_out = jnp.where(at_pos, rope_new[:, None, :], rope_cache)

    def one_token(item_tuple):
        q_lat_t, q_rope_t, lat_t, rope_t, pos_t = item_tuple
        scores = jnp.dot(q_lat_t, lat_t.T, preferred_element_type=jnp.float32)
        scores = scores + jnp.dot(q_rope_t, rope_t.T, preferred_element_type=jnp.float32)
        scores = scores * ATTN_SCALE
        visible = seq_ids[None, :] <= pos_t
        scores = jnp.where(visible, scores, -jnp.inf)
        prob_mat = jax.nn.softmax(scores, axis=-1).astype(jnp.bfloat16)
        return jnp.dot(prob_mat, lat_t, preferred_element_type=jnp.float32).astype(jnp.bfloat16)

    o_lat = lax.map(one_token, (q_lat, q_rope, lat_out, rope_out, tok_pos))
    o_heads = jnp.einsum('bhc,hcv->bhv', o_lat.astype(jnp.float32), w_uval.astype(jnp.float32)).astype(jnp.bfloat16)
    attn_out = jnp.dot(o_heads.reshape(NUM_TOKENS, NUM_HEADS * V_DIM), w_out, preferred_element_type=jnp.float32)
    resid_bf = (x_wide + attn_out).astype(jnp.bfloat16)
    h_norm = rms_norm(resid_bf.astype(jnp.float32), ffn_gain).astype(jnp.bfloat16)
    gate_prob = jax.nn.sigmoid(jnp.dot(h_norm, w_router, preferred_element_type=jnp.float32))
    chosen = jnp.take_along_axis(gate_prob, expert_ids, axis=1)
    route_w = ROUTE_SCALE * chosen / jnp.sum(chosen, axis=1, keepdims=True)
    sh_act = (jax.nn.silu(jnp.dot(h_norm, sh_gate, preferred_element_type=jnp.float32)) * jnp.dot(h_norm, sh_up, preferred_element_type=jnp.float32)).astype(jnp.bfloat16)
    shared_out = jnp.dot(sh_act, sh_down, preferred_element_type=jnp.float32)
    flat_rows = jnp.repeat(h_norm, TOP_K, axis=0)
    flat_ids = expert_ids.reshape(NUM_TOKENS * TOP_K)

    def one_choice(item_tuple):
        row_vec, expert = item_tuple
        row_mat = row_vec[None, :]
        gate_val = jnp.dot(row_mat, ex_gate[expert], preferred_element_type=jnp.float32)
        up_val = jnp.dot(row_mat, ex_up[expert], preferred_element_type=jnp.float32)
        act_val = (jax.nn.silu(gate_val) * up_val).astype(jnp.bfloat16)
        return jnp.dot(act_val, ex_down[expert], preferred_element_type=jnp.float32).astype(jnp.bfloat16)[0]

    choice_out = lax.map(one_choice, (flat_rows, flat_ids)).reshape(NUM_TOKENS, TOP_K, D_MODEL)
    routed = jnp.sum(route_w[:, :, None] * choice_out.astype(jnp.float32), axis=1)
    out_hidden = (resid_bf.astype(jnp.float32) + shared_out + routed).astype(jnp.bfloat16)
    return (out_hidden, lat_out, rope_out)
```

```python
import functools

import jax
import jax.numpy as jnp
import numpy as np
from jax import lax
from jax.experimental import pallas as pl
from jax.experimental.pallas import tpu as pltpu
from jax.sharding import PartitionSpec as P

ROUTE_SCALE = 2.827
ROPE_BASE = 10000.0
NORM_EPS = 1e-6
MESH = pl.DeviceIdType.MESH
F32 = jnp.float32
BF16 = jnp.bfloat16
CHUNKS = 4
SLOTS_A = 6
SLOTS_B = 8
CAP = 6
LANES = 128


def unit_norm(values):
    mean_sq = jnp.mean(jnp.square(values), axis=-1, keepdims=True)
    return values * lax.rsqrt(mean_sq + NORM_EPS)


def rms_norm(values, gain_vec):
    return unit_norm(values) * gain_vec.astype(jnp.float32)


def rope_rotate(values, angle_rad):
    half_dim = values.shape[-1] // 2
    x_first = values[..., :half_dim]
    x_second = values[..., half_dim:]
    cos_part = jnp.cos(angle_rad)
    sin_part = jnp.sin(angle_rad)
    return jnp.concatenate([x_first * cos_part - x_second * sin_part, x_second * cos_part + x_first * sin_part], axis=-1)


def attention_block(tok_in, lat_cache, rope_cache, tok_pos, attn_gain, w_query, w_kvdown, w_ukey, w_uval, w_out, ffn_gain):
    num_heads, nope_dim, kv_rank = w_ukey.shape
    rope_dim = rope_cache.shape[-1]
    seq_len = lat_cache.shape[1]
    tok_rows = tok_in.shape[0]
    x_wide = tok_in.astype(jnp.float32)
    x_norm = rms_norm(x_wide, attn_gain).astype(jnp.bfloat16)
    q_all = jnp.dot(x_norm, w_query, preferred_element_type=jnp.float32).astype(jnp.bfloat16).reshape(tok_rows, num_heads, nope_dim + rope_dim)
    kv_all = jnp.dot(x_norm, w_kvdown, preferred_element_type=jnp.float32)
    inv_freq = ROPE_BASE ** (-(2.0 * jnp.arange(rope_dim // 2)) / rope_dim)
    angle_rad = tok_pos.astype(jnp.float32)[:, None] * inv_freq[None, :]
    lat_new = unit_norm(kv_all[:, :kv_rank]).astype(jnp.bfloat16)
    rope_new = rope_rotate(kv_all[:, kv_rank:], angle_rad).astype(jnp.bfloat16)
    q_rope = rope_rotate(q_all[:, :, nope_dim:].astype(jnp.float32), angle_rad[:, None, :]).astype(jnp.bfloat16)
    q_lat = jnp.einsum('bhn,hnc->bhc', q_all[:, :, :nope_dim], w_ukey, preferred_element_type=jnp.float32).astype(jnp.bfloat16)
    seq_ids = jnp.arange(seq_len)
    at_pos = (seq_ids[None, :] == tok_pos[:, None])[:, :, None]
    lat_out = jnp.where(at_pos, lat_new[:, None, :], lat_cache)
    rope_out = jnp.where(at_pos, rope_new[:, None, :], rope_cache)
    scores = jnp.einsum('bhc,bsc->bhs', q_lat, lat_out, preferred_element_type=jnp.float32)
    scores = scores + jnp.einsum('bhr,bsr->bhs', q_rope, rope_out, preferred_element_type=jnp.float32)
    scores = scores * (nope_dim + rope_dim) ** -0.5
    visible = (seq_ids[None, :] <= tok_pos[:, None])[:, None, :]
    scores = jnp.where(visible, scores, -jnp.inf)
    prob_mat = jax.nn.softmax(scores, axis=-1).astype(jnp.bfloat16)
    o_lat = jnp.einsum('bhs,bsc->bhc', prob_mat, lat_out, preferred_element_type=jnp.float32).astype(jnp.bfloat16)
    o_heads = jnp.einsum('bhc,hcv->bhv', o_lat, w_uval, preferred_element_type=jnp.float32).astype(jnp.bfloat16)
    attn_out = jnp.dot(o_heads.reshape(tok_rows, -1), w_out, preferred_element_type=jnp.float32)
    resid_bf = (x_wide + attn_out).astype(jnp.bfloat16)
    h_norm = rms_norm(resid_bf.astype(jnp.float32), ffn_gain).astype(jnp.bfloat16)
    return resid_bf, h_norm, lat_out, rope_out


def route_table(h_norm, w_router, expert_ids):
    num_experts = w_router.shape[1]
    tok_rows = expert_ids.shape[0]
    gate_prob = jax.nn.sigmoid(jnp.dot(h_norm, w_router, preferred_element_type=jnp.float32))
    listed = jnp.sum((expert_ids[:, :, None] == jnp.arange(num_experts)[None, None, :]).astype(F32), axis=1)
    chosen = gate_prob * listed
    weights = ROUTE_SCALE * chosen / jnp.sum(chosen, axis=1, keepdims=True)
    earlier = jnp.tril(jnp.ones((tok_rows, tok_rows), F32))
    slots = jnp.dot(earlier, listed, preferred_element_type=F32) * listed
    return jnp.concatenate([weights, slots], axis=1)


def dot32(lhs, rhs):
    return jnp.dot(lhs, rhs, preferred_element_type=F32)


def wide_tiles(total, width):
    return [(start, min(width, total - start)) for start in range(0, total, width)]


def moe_kernel(n_ep, n_exp, h_ref, table_ref, resid_ref, rowpat_ref, colpat_ref,
               sg_ref, su_ref, sd_ref, eg_ref, eu_ref, ed_ref, out_ref,
               hall, gall, xg, act, act_sh, ebuf, esib, cmat, ct, ring, wa, wb, sh_out,
               sem_a, sem_b, ag_send, ag_recv, sib_send, sib_recv, tb_send, tb_recv, ts_send, ts_recv,
               ex_send, ex_recv, rg_send, rg_recv):
    nz = n_ep // 2
    far = nz // 2
    tok, dim = h_ref.shape
    e_loc, _, ff = eg_ref.shape
    halves = sg_ref.shape[1] // ff
    rows_par = nz * CAP
    rows_exp = 2 * rows_par
    rows_all = e_loc * rows_exp
    rows_q = e_loc * rows_par
    cw = dim // CHUNKS
    half_dim = dim // 2

    me = lax.axis_index('ep')
    z = me // 2
    par = lax.rem(me, 2)
    sib = me + 1 - 2 * par
    up_dev = lax.rem(z + 1, nz) * 2 + par
    dn_dev = lax.rem(z + nz - 1, nz) * 2 + par

    def chip(step):
        return lax.rem(z + step + 2 * nz, nz)

    def slot_of(p, zz):
        return p * nz + zz

    total_a = 2 * e_loc + 2 * halves

    def a_copy(unit, expert=None):
        slot = unit % SLOTS_A
        if unit < 2 * e_loc:
            src = (eg_ref if unit % 2 == 0 else eu_ref).at[unit // 2]
        else:
            hf = (unit - 2 * e_loc) // 2
            src = (sg_ref if unit % 2 == 0 else su_ref).at[:, pl.ds(hf * ff, ff)]
        return pltpu.make_async_copy(src, wa.at[slot], sem_a.at[slot])

    total_b = CHUNKS * (e_loc + halves)

    def b_copy(unit):
        slot = unit % SLOTS_B
        if unit < CHUNKS * e_loc:
            j, e = unit // e_loc, unit % e_loc
            src = ed_ref.at[e, :, pl.ds(j * cw, cw)]
        else:
            j, hf = (unit - CHUNKS * e_loc) // halves, (unit - CHUNKS * e_loc) % halves
            src = sd_ref.at[pl.ds(hf * ff, ff), pl.ds(j * cw, cw)]
        return pltpu.make_async_copy(src, wb.at[slot], sem_b.at[slot])

    for unit in range(min(SLOTS_A, total_a)):
        a_copy(unit).start()

    barrier = pltpu.get_barrier_semaphore()
    for dev in (up_dev, dn_dev, sib):
        pl.semaphore_signal(barrier, inc=1, device_id={'ep': dev}, device_id_type=MESH)
    pl.semaphore_wait(barrier, 3)

    def remote(src, dst, send, recv, dev):
        return pltpu.make_async_remote_copy(src_ref=src, dst_ref=dst, send_sem=send, recv_sem=recv,
                                            device_id={'ep': dev}, device_id_type=MESH)

    def h_hop(way, step):
        dev = up_dev if way == 0 else dn_dev
        origin = chip(-step if way == 0 else step)
        slot = slot_of(par, origin)
        if step == far - 1:
            cols = pl.ds(way * half_dim, half_dim)
            src, dst = hall.at[slot, :, cols], hall.at[slot, :, cols]
        else:
            src = h_ref if step == 0 else hall.at[slot]
            dst = hall.at[slot]
        return remote(src, dst, ag_send.at[way, step], ag_recv.at[way, step], dev)

    def t_hop(way, step):
        dev = up_dev if way == 0 else dn_dev
        origin = chip(-step if way == 0 else step)
        slot = slot_of(par, origin)
        src = table_ref if step == 0 else gall.at[slot]
        return remote(src, gall.at[slot], tb_send.at[way, step], tb_recv.at[way, step], dev)

    def h_cross(k, origin):
        slot = slot_of(par, origin)
        src = h_ref if k == 0 else hall.at[slot]
        return remote(src, hall.at[slot], sib_send.at[k], sib_recv.at[k], sib)

    def t_cross(k, origin):
        slot = slot_of(par, origin)
        src = table_ref if k == 0 else gall.at[slot]
        return remote(src, gall.at[slot], ts_send.at[k], ts_recv.at[k], sib)

    t_steps = (far, far - 1)
    sent = []

    def go(copy):
        copy.start()
        sent.append(copy)
        return copy

    hops = [[None] * far, [None] * far]
    thops = [[None] * far, [None] * far]
    for way in range(2):
        thops[way][0] = go(t_hop(way, 0))
        hops[way][0] = go(h_hop(way, 0))
    crossed = [go(t_cross(0, z)), go(h_cross(0, z))]
    hall[slot_of(par, z)] = h_ref[...]
    gall[slot_of(par, z)] = table_ref[...]
    k = 1
    for step in range(far):
        for way in range(2):
            origin = chip(-(step + 1) if way == 0 else step + 1)
            if step < t_steps[way]:
                thops[way][step].wait_recv()
                if step + 1 < t_steps[way]:
                    thops[way][step + 1] = go(t_hop(way, step + 1))
                crossed.append(go(t_cross(k if step < far - 1 else 2 * far - 1, origin)))
            hops[way][step].wait_recv()
            if step + 1 < far:
                hops[way][step + 1] = go(h_hop(way, step + 1))
                crossed.append(go(h_cross(k, origin)))
                k += 1
    crossed.append(go(h_cross(2 * far - 1, chip(far))))
    for copy in crossed:
        copy.wait_recv()

    rowpat = rowpat_ref[...]
    row_exp, row_dev, row_slot = rowpat[:, 0:1], rowpat[:, 1:2], rowpat[:, 2:3]
    base = n_exp + e_loc * me
    lane = lax.broadcasted_iota(jnp.int32, (rows_all, LANES), 1)
    pick = jnp.where(lane == base + row_exp.astype(jnp.int32), 1.0, 0.0).astype(BF16)
    slots_by_row = lax.dot_general(pick, gall[...].reshape(n_ep * tok, LANES).astype(BF16), (((1,), (1,)), ((), ())),
                                   preferred_element_type=F32)
    tok_dev = (lax.broadcasted_iota(jnp.int32, (rows_all, n_ep * tok), 1) // tok).astype(F32)
    place = jnp.where((slots_by_row == row_slot) & (tok_dev == row_dev), 1.0, 0.0).astype(BF16)
    for start, width in wide_tiles(dim, 256):
        rows = hall[:, :, start:start + width].reshape(n_ep * tok, width)
        xg[:, :, start:start + width] = dot32(place, rows).astype(BF16).reshape(e_loc, rows_exp, width)

    colpat = colpat_ref[...]
    col_exp, col_chip, col_slot = colpat[0:1, :], colpat[1:2, :], colpat[2:3, :]
    g_own = gall[pl.ds(par * nz, nz)].reshape(nz * tok, LANES)
    part1 = g_own.astype(BF16)
    rest1 = g_own - part1.astype(F32)
    part2 = rest1.astype(BF16)
    part3 = (rest1 - part2.astype(F32)).astype(BF16)
    sub = lax.broadcasted_iota(jnp.int32, (LANES, rows_q), 0)
    tok_chip = (lax.broadcasted_iota(jnp.int32, (nz * tok, rows_q), 0) // tok).astype(F32)
    for q in range(2):
        ids = e_loc * (me if q == 0 else sib) + col_exp.astype(jnp.int32)
        sel_w = jnp.where(sub == ids, 1.0, 0.0).astype(BF16)
        sel_s = jnp.where(sub == n_exp + ids, 1.0, 0.0).astype(BF16)
        here = (dot32(part1, sel_s) == col_slot) & (tok_chip == col_chip)
        for i, part in enumerate((part1, part2, part3)):
            cmat[q, i] = jnp.where(here, dot32(part, sel_w), 0.0).astype(BF16)

    def swiglu_tiles(x, slot_g, slot_u, store):
        for start, width in wide_tiles(ff, 256):
            gate = dot32(x, wa[slot_g, :, start:start + width])
            up = dot32(x, wa[slot_u, :, start:start + width])
            store(start, width, (jax.nn.silu(gate) * up).astype(BF16))

    def wait_a(slot):
        pltpu.make_async_copy(eg_ref.at[0], wa.at[slot], sem_a.at[slot]).wait()

    def wait_b(slot):
        pltpu.make_async_copy(ed_ref.at[0, :, pl.ds(0, cw)], wb.at[slot], sem_b.at[slot]).wait()

    def expert_up(e, carry):
        slot_g = lax.rem(2 * e, SLOTS_A)
        slot_u = lax.rem(2 * e + 1, SLOTS_A)
        wait_a(slot_g)
        wait_a(slot_u)

        def store(start, width, val):
            act[e, :, start:start + width] = val
        swiglu_tiles(xg[e], slot_g, slot_u, store)
        for e_st in range(e_loc):
            @pl.when(e == e_st)
            def _():
                for unit in (2 * e_st + SLOTS_A, 2 * e_st + 1 + SLOTS_A):
                    if unit < 2 * e_loc:
                        a_copy(unit).start()
                if e_st == 0:
                    for unit in range(SLOTS_B):
                        b_copy(unit).start()
                for unit in (2 * e_st + SLOTS_A, 2 * e_st + 1 + SLOTS_A):
                    if 2 * e_loc <= unit < total_a:
                        a_copy(unit).start()
        return carry

    lax.fori_loop(0, e_loc, expert_up, 0)

    def reach(way, j):
        return far if (way + j) % 2 == 0 else nz - 1 - far

    def ring_copy(way, j, step):
        dev = up_dev if way == 0 else dn_dev
        ahead = reach(way, j) - step + 1
        dest = chip(ahead if way == 0 else -ahead)
        src = ct.at[j, dest] if step == 1 else ring.at[way, j, step - 2]
        return remote(src, ring.at[way, j, step - 1], rg_send.at[way, j, step - 1], rg_recv.at[way, j, step - 1], dev)

    rcopies = {}

    def combine(j):
        exch[j].wait_recv()
        own = ebuf[j, par].reshape(rows_q, cw)
        other = esib[j].reshape(rows_q, cw)
        for start, width in wide_tiles(cw, 256):
            total = dot32(cmat[0, 0], own[:, start:start + width]) + dot32(cmat[1, 0], other[:, start:start + width])
            for i in (1, 2):
                total += dot32(cmat[0, i], own[:, start:start + width]) + dot32(cmat[1, i], other[:, start:start + width])
            ct[j, :, :, start:start + width] = total.reshape(nz, tok, width)
        for way in range(2):
            rcopies[way, j, 1] = go(ring_copy(way, j, 1))

    def advance(j, step):
        for way in range(2):
            if step < reach(way, j):
                rcopies[way, j, step].wait_recv()
                ahead = reach(way, j) - step
                dest = chip(ahead if way == 0 else -ahead)
                ring[way, j, step - 1] += ct[j, dest]
                rcopies[way, j, step + 1] = go(ring_copy(way, j, step + 1))

    def finish(j):
        cols = slice(j * cw, (j + 1) * cw)
        total = resid_ref[:, cols].astype(F32) + sh_out[:, cols] + ct[j, z]
        for way in range(2):
            rcopies[way, j, reach(way, j)].wait_recv()
            total += ring[way, j, reach(way, j) - 1]
        out_ref[:, cols] = total.astype(BF16)

    exch = {}

    def down(j):
        def one(e, carry):
            slot = lax.rem(j * e_loc + e, SLOTS_B)
            wait_b(slot)
            res = dot32(act[e], wb[slot]).astype(BF16)
            ebuf[j, 0, e] = res[:rows_par]
            ebuf[j, 1, e] = res[rows_par:]
            return carry
        lax.fori_loop(0, e_loc, one, 0)
        for e in range(e_loc):
            unit = j * e_loc + e + SLOTS_B
            if unit < total_b:
                b_copy(unit).start()
        exch[j] = go(remote(ebuf.at[j, 1 - par], esib.at[j], ex_send.at[j], ex_recv.at[j], sib))

    def shared_up(hf):
        unit = 2 * e_loc + 2 * hf
        wait_a(unit % SLOTS_A)
        wait_a((unit + 1) % SLOTS_A)

        def store(start, width, val):
            act_sh[hf, :, start:start + width] = val
        swiglu_tiles(h_ref[...], unit % SLOTS_A, (unit + 1) % SLOTS_A, store)

    def shared_down(j):
        total = jnp.zeros((tok, cw), F32)
        for hf in range(halves):
            unit = CHUNKS * e_loc + j * halves + hf
            wait_b(unit % SLOTS_B)
            total += dot32(act_sh[hf], wb[unit % SLOTS_B])
        sh_out[:, j * cw:(j + 1) * cw] = total
        for hf in range(halves):
            unit = CHUNKS * e_loc + j * halves + hf + SLOTS_B
            if unit < total_b:
                b_copy(unit).start()

    down(0)
    down(1)
    combine(0)
    down(2)
    combine(1)
    advance(0, 1)
    down(3)
    combine(2)
    advance(1, 1)
    combine(3)
    advance(0, 2)
    shared_up(0)
    advance(2, 1)
    advance(1, 2)
    advance(3, 1)
    shared_up(1)
    advance(0, 3)
    advance(2, 2)
    shared_down(0)
    advance(1, 3)
    advance(3, 2)
    shared_down(1)
    advance(2, 3)
    shared_down(2)
    advance(3, 3)
    shared_down(3)
    for j in range(CHUNKS):
        finish(j)
    for copy in sent:
        copy.wait_send()


def moe_call(n_ep, h_norm, table, resid, w_sg, w_su, w_sd, w_eg, w_eu, w_ed):
    nz = n_ep // 2
    tok, dim = h_norm.shape
    e_loc, _, ff = w_eg.shape
    n_exp = e_loc * n_ep
    halves = w_sg.shape[1] // ff
    far = nz // 2
    cw = dim // CHUNKS
    rows_par = nz * CAP
    rows_exp = 2 * rows_par
    rows_all = e_loc * rows_exp
    rows_q = e_loc * rows_par
    row = np.arange(rows_all)
    rowpat = np.zeros((rows_all, 8), np.float32)
    rowpat[:, 0] = row // rows_exp
    rowpat[:, 1] = (row % rows_exp) // CAP
    rowpat[:, 2] = row % CAP + 1
    col = np.arange(rows_q)
    colpat = np.zeros((8, rows_q), np.float32)
    colpat[0] = col // rows_par
    colpat[1] = (col % rows_par) // CAP
    colpat[2] = col % CAP + 1
    vmem = pl.BlockSpec(memory_space=pltpu.VMEM)
    hbm = pl.BlockSpec(memory_space=pl.ANY)
    dma = pltpu.SemaphoreType.DMA
    return pl.pallas_call(
        functools.partial(moe_kernel, n_ep, n_exp),
        out_shape=jax.ShapeDtypeStruct((tok, dim), BF16),
        in_specs=[vmem] * 5 + [hbm] * 6,
        out_specs=vmem,
        scratch_shapes=[
            pltpu.VMEM((n_ep, tok, dim), BF16),
            pltpu.VMEM((n_ep, tok, LANES), F32),
            pltpu.VMEM((e_loc, rows_exp, dim), BF16),
            pltpu.VMEM((e_loc, rows_exp, ff), BF16),
            pltpu.VMEM((halves, tok, ff), BF16),
            pltpu.VMEM((CHUNKS, 2, e_loc, rows_par, cw), BF16),
            pltpu.VMEM((CHUNKS, e_loc, rows_par, cw), BF16),
            pltpu.VMEM((2, 3, nz * tok, rows_q), BF16),
            pltpu.VMEM((CHUNKS, nz, tok, cw), F32),
            pltpu.VMEM((2, CHUNKS, far, tok, cw), F32),
            pltpu.VMEM((SLOTS_A, dim, ff), BF16),
            pltpu.VMEM((SLOTS_B, ff, cw), BF16),
            pltpu.VMEM((tok, dim), F32),
            dma((SLOTS_A,)), dma((SLOTS_B,)),
            dma((2, far)), dma((2, far)), dma((nz,)), dma((nz,)),
            dma((2, far)), dma((2, far)), dma((nz,)), dma((nz,)),
            dma((CHUNKS,)), dma((CHUNKS,)),
            dma((2, CHUNKS, far)), dma((2, CHUNKS, far)),
        ],
        compiler_params=pltpu.CompilerParams(collective_id=0, has_side_effects=True, vmem_limit_bytes=67000000),
        name='moe_ring',
    )(h_norm, table, resid, jnp.asarray(rowpat), jnp.asarray(colpat), w_sg, w_su, w_sd, w_eg, w_eu, w_ed)


def solution(mesh):
    n_ep = mesh.shape['ep']
    row_one = P(('dp', 'ep'))
    row_two = P(('dp', 'ep'), None)
    row_three = P(('dp', 'ep'), None, None)
    rep_one = P(None)
    rep_two = P(None, None)
    rep_three = P(None, None, None)
    exp_spec = P('ep', None, None)

    def local_step(tok_in, lat_cache, rope_cache, tok_pos, expert_ids, attn_gain, w_query, w_kvdown, w_ukey, w_uval, w_out, ffn_gain, w_router, sh_gate, sh_up, sh_down, ex_gate, ex_up, ex_down):
        resid_bf, h_norm, lat_out, rope_out = attention_block(tok_in, lat_cache, rope_cache, tok_pos, attn_gain, w_query, w_kvdown, w_ukey, w_uval, w_out, ffn_gain)
        table = route_table(h_norm, w_router, expert_ids)
        out_hidden = moe_call(n_ep, h_norm, table, resid_bf, sh_gate, sh_up, sh_down, ex_gate, ex_up, ex_down)
        return out_hidden, lat_out, rope_out

    in_specs = (row_two, row_three, row_three, row_one, row_two, rep_one, rep_two, rep_two, rep_three, rep_three, rep_two, rep_one, rep_two, rep_two, rep_two, rep_two, exp_spec, exp_spec, exp_spec)
    out_specs = (row_two, row_three, row_three)
    return jax.shard_map(local_step, mesh=mesh, in_specs=in_specs, out_specs=out_specs, check_vma=False)
```

```python
import functools

import jax
import jax.numpy as jnp
import numpy as np
from jax import lax
from jax.experimental import pallas as pl
from jax.experimental.pallas import tpu as pltpu
from jax.sharding import PartitionSpec as P

ROUTE_SCALE = 2.827
ROPE_BASE = 10000.0
NORM_EPS = 1e-6
MESH = pl.DeviceIdType.MESH
F32 = jnp.float32
BF16 = jnp.bfloat16
CHUNKS = 4
SLOTS_A = 7
SLOTS_B = 4
CAP = 6
LANES = 128
GROUP = 4


def unit_norm(values):
    mean_sq = jnp.mean(jnp.square(values), axis=-1, keepdims=True)
    return values * lax.rsqrt(mean_sq + NORM_EPS)


def dot32(lhs, rhs):
    return jnp.dot(lhs, rhs, preferred_element_type=F32)


def wide_tiles(total, width):
    return [(start, min(width, total - start)) for start in range(0, total, width)]


def attn_kernel(pos_ref, x_ref, trig_ref, ids_ref, ag_ref, fg_ref, wq_ref, wkv_ref, uk_ref, uv_ref, wo_ref, wr_ref, lat_ref, rope_ref,
                res_ref, h_ref, table_ref, lat_out, rope_out,
                wq, wkv, uk, uv, wo, wr, lat, rope, q_lat, q_rope, o_lat, o_heads, sem_q, sem_w, sem_c, sem_o):
    n_heads, nope, rank = uk_ref.shape
    tok, dim = x_ref.shape
    seq, rope_dim = rope_ref.shape[1:]
    half = rope_dim // 2
    head = nope + rope_dim
    n_exp = wr_ref.shape[1]
    blocks = n_heads // GROUP
    q_cols = GROUP * head

    def q_copy(blk):
        return pltpu.make_async_copy(wq_ref.at[:, pl.ds(blk * q_cols, q_cols)], wq.at[blk], sem_q.at[blk])

    kv_copy = pltpu.make_async_copy(wkv_ref, wkv, sem_w.at[0])
    uk_copy = pltpu.make_async_copy(uk_ref, uk, sem_w.at[1])
    uv_copy = pltpu.make_async_copy(uv_ref, uv, sem_w.at[2])
    wo_copy = pltpu.make_async_copy(wo_ref, wo, sem_w.at[3])
    wr_copy = pltpu.make_async_copy(wr_ref, wr, sem_w.at[4])
    lat_copy = pltpu.make_async_copy(lat_ref, lat, sem_c.at[0])
    rope_copy = pltpu.make_async_copy(rope_ref, rope, sem_c.at[1])
    kv_copy.start()
    lat_copy.start()
    rope_copy.start()
    uk_copy.start()
    for blk in range(blocks):
        q_copy(blk).start()
    uv_copy.start()
    wr_copy.start()
    wo_copy.start()

    x = x_ref[...].astype(F32)
    x_norm = (unit_norm(x) * ag_ref[...].astype(F32)).astype(BF16)
    cos, sin = trig_ref[:, :half], trig_ref[:, half:]

    def rotate(first, second):
        return jnp.concatenate([first * cos - second * sin, second * cos + first * sin], axis=1)

    kv_copy.wait()
    kv = dot32(x_norm, wkv[...])
    lat_new = unit_norm(kv[:, :rank]).astype(BF16).astype(F32)
    rope_new = rotate(kv[:, rank:rank + half], kv[:, rank + half:]).astype(BF16).astype(F32)
    lat_copy.wait()
    rope_copy.wait()
    for t in range(tok):
        here = lax.broadcasted_iota(jnp.int32, (seq, rank), 0) == pos_ref[t]
        lat[t] = jnp.where(here, lat_new[t:t + 1], lat[t].astype(F32)).astype(BF16)
        here = lax.broadcasted_iota(jnp.int32, (seq, rope_dim), 0) == pos_ref[t]
        rope[t] = jnp.where(here, rope_new[t:t + 1], rope[t].astype(F32)).astype(BF16)
    lat_back = pltpu.make_async_copy(lat, lat_out, sem_o.at[0])
    rope_back = pltpu.make_async_copy(rope, rope_out, sem_o.at[1])

    def spread(ref, n, val):
        for c in range(val.shape[1] // LANES):
            ref[c, pl.ds(n, tok, stride=n_heads), :] = val[:, c * LANES:(c + 1) * LANES]

    uk_copy.wait()
    for blk in range(blocks):
        q_copy(blk).wait()
        q = dot32(x_norm, wq[blk]).astype(BF16)
        for i in range(GROUP):
            n = blk * GROUP + i
            at = i * head
            q_n = dot32(q[:, at:at + nope], uk[n]).astype(BF16).astype(F32)
            spread(q_lat, n, q_n)
            q_r = q[:, at + nope:at + head].astype(F32)
            q_r = rotate(q_r[:, :half], q_r[:, half:]).astype(BF16).astype(F32)
            spread(q_rope, n, jnp.concatenate([q_r, jnp.zeros((tok, LANES - rope_dim), F32)], axis=1))
    lat_back.start()
    rope_back.start()

    rows, keys = GROUP * n_heads, GROUP * seq
    key = lax.broadcasted_iota(jnp.int32, (rows, keys), 1)
    same = (key // seq) == (lax.broadcasted_iota(jnp.int32, (rows, keys), 0) // n_heads)
    key_tok, key_seq = key // seq, lax.rem(key, seq)
    across = (((1,), (1,)), ((), ()))
    for g in range(tok // GROUP):
        lat_g = lat[g * GROUP:(g + 1) * GROUP].reshape(keys, rank)
        rope_g = rope[g * GROUP:(g + 1) * GROUP].reshape(keys, rope_dim)
        sl = slice(g * rows, (g + 1) * rows)
        scores = lax.dot_general(jnp.concatenate([q_lat[c, sl] for c in range(rank // LANES)], axis=1).astype(BF16), lat_g, across, preferred_element_type=F32)
        scores = scores + lax.dot_general(q_rope[0, sl, :rope_dim].astype(BF16), rope_g, across, preferred_element_type=F32)
        scores = scores * head ** -0.5
        last = jnp.full((rows, keys), pos_ref[g * GROUP], jnp.int32)
        for i in range(1, GROUP):
            last = jnp.where(key_tok == i, pos_ref[g * GROUP + i], last)
        scores = jnp.where(same & (key_seq <= last), scores, -jnp.inf)
        top = jnp.max(scores, axis=1, keepdims=True)
        expd = jnp.exp(scores - top)
        probs = (expd / jnp.sum(expd, axis=1, keepdims=True)).astype(BF16)
        o_g = dot32(probs, lat_g).astype(BF16).astype(F32)
        for c in range(rank // LANES):
            o_lat[c, sl] = o_g[:, c * LANES:(c + 1) * LANES]

    uv_copy.wait()
    for n in range(n_heads):
        o_n = jnp.concatenate([o_lat[c, pl.ds(n, tok, stride=n_heads), :] for c in range(rank // LANES)], axis=1).astype(BF16)
        o_heads[:, n * uv.shape[2]:(n + 1) * uv.shape[2]] = dot32(o_n, uv[n]).astype(BF16)
    wr_copy.wait()
    wo_copy.wait()
    for start, width in wide_tiles(dim, 512):
        attn = dot32(o_heads[...], wo[:, start:start + width])
        res_ref[:, start:start + width] = (x[:, start:start + width] + attn).astype(BF16)
    h = (unit_norm(res_ref[...].astype(F32)) * fg_ref[...].astype(F32)).astype(BF16)
    h_ref[...] = h

    gate = jax.nn.sigmoid(dot32(h, wr[...]))
    ids = ids_ref[...]
    exp_lane = lax.broadcasted_iota(jnp.int32, (tok, n_exp), 1)
    listed = jnp.zeros((tok, n_exp), F32)
    for i in range(ids_ref.shape[1]):
        listed = listed + jnp.where(exp_lane == ids[:, i:i + 1], 1.0, 0.0)
    lower = lax.broadcasted_iota(jnp.int32, (tok, tok), 0) >= lax.broadcasted_iota(jnp.int32, (tok, tok), 1)
    slots = dot32(jnp.where(lower, 1.0, 0.0).astype(BF16), listed.astype(BF16)) * listed
    chosen = gate * listed
    table_ref[:, :n_exp] = ROUTE_SCALE * chosen / jnp.sum(chosen, axis=1, keepdims=True)
    table_ref[:, n_exp:] = slots
    lat_back.wait()
    rope_back.wait()


def attn_call(tok_in, lat_cache, rope_cache, tok_pos, expert_ids, attn_gain, w_query, w_kvdown, w_ukey, w_uval, w_out, ffn_gain, w_router):
    tok, dim = tok_in.shape
    n_heads, nope, rank = w_ukey.shape
    seq, rope_dim = rope_cache.shape[1:]
    n_exp = w_router.shape[1]
    blocks = n_heads // GROUP
    inv_freq = ROPE_BASE ** (-(2.0 * jnp.arange(rope_dim // 2)) / rope_dim)
    angle = tok_pos.astype(F32)[:, None] * inv_freq[None, :]
    trig = jnp.concatenate([jnp.cos(angle), jnp.sin(angle)], axis=1)
    vmem = pl.BlockSpec(memory_space=pltpu.VMEM)
    hbm = pl.BlockSpec(memory_space=pl.ANY)
    dma = pltpu.SemaphoreType.DMA
    return pl.pallas_call(
        attn_kernel,
        out_shape=[
            jax.ShapeDtypeStruct((tok, dim), BF16),
            jax.ShapeDtypeStruct((tok, dim), BF16),
            jax.ShapeDtypeStruct((tok, 2 * n_exp), F32),
            jax.ShapeDtypeStruct(lat_cache.shape, BF16),
            jax.ShapeDtypeStruct(rope_cache.shape, BF16),
        ],
        in_specs=[pl.BlockSpec(memory_space=pltpu.SMEM)] + [vmem] * 5 + [hbm] * 8,
        out_specs=[vmem, vmem, vmem, hbm, hbm],
        scratch_shapes=[
            pltpu.VMEM((blocks, dim, w_query.shape[1] // blocks), BF16),
            pltpu.VMEM(w_kvdown.shape, BF16),
            pltpu.VMEM(w_ukey.shape, BF16),
            pltpu.VMEM(w_uval.shape, BF16),
            pltpu.VMEM(w_out.shape, BF16),
            pltpu.VMEM(w_router.shape, BF16),
            pltpu.VMEM(lat_cache.shape, BF16),
            pltpu.VMEM(rope_cache.shape, BF16),
            pltpu.VMEM((rank // LANES, tok * n_heads, LANES), F32),
            pltpu.VMEM((1, tok * n_heads, LANES), F32),
            pltpu.VMEM((rank // LANES, tok * n_heads, LANES), F32),
            pltpu.VMEM((tok, w_out.shape[0]), BF16),
            dma((blocks,)), dma((5,)), dma((2,)), dma((2,)),
        ],
        compiler_params=pltpu.CompilerParams(vmem_limit_bytes=60000000),
        name='latent_attention',
    )(tok_pos, tok_in, trig, expert_ids, attn_gain[None, :], ffn_gain[None, :], w_query, w_kvdown, w_ukey, w_uval, w_out, w_router, lat_cache, rope_cache)


def moe_kernel(n_ep, n_exp, h_ref, table_ref, resid_ref, rowpat_ref, colpat_ref,
               sg_ref, su_ref, sd_ref, eg_ref, eu_ref, ed_ref, out_ref,
               hall, gall, xg, act, act_sh, ebuf, esib, cmat, ct, ring, wa, wb, sh_out,
               sem_a, sem_b, ag_send, ag_recv, sib_send, sib_recv, tb_send, tb_recv, ts_send, ts_recv,
               ex_send, ex_recv, rg_send, rg_recv):
    nz = n_ep // 2
    far = nz // 2
    tok, dim = h_ref.shape
    e_loc, _, ff = eg_ref.shape
    halves = sg_ref.shape[1] // ff
    rows_par = nz * CAP
    rows_exp = 2 * rows_par
    rows_all = e_loc * rows_exp
    rows_q = e_loc * rows_par
    cw = dim // CHUNKS
    half_dim = dim // 2

    me = lax.axis_index('ep')
    z = me // 2
    par = lax.rem(me, 2)
    sib = me + 1 - 2 * par
    up_dev = lax.rem(z + 1, nz) * 2 + par
    dn_dev = lax.rem(z + nz - 1, nz) * 2 + par

    def chip(step):
        return lax.rem(z + step + 2 * nz, nz)

    def slot_of(p, zz):
        return p * nz + zz

    def a_slot(unit):
        return unit % SLOTS_A if unit < 2 * e_loc else unit - 2 * e_loc

    def a_copy(unit):
        slot = a_slot(unit)
        if unit < 2 * e_loc:
            src = (eg_ref if unit % 2 == 0 else eu_ref).at[unit // 2]
        else:
            hf = (unit - 2 * e_loc) // 2
            src = (sg_ref if unit % 2 == 0 else su_ref).at[:, pl.ds(hf * ff, ff)]
        return pltpu.make_async_copy(src, wa.at[slot], sem_a.at[unit])

    def b_place(unit):
        if unit >= CHUNKS * e_loc + SLOTS_B:
            pos = unit - CHUNKS * e_loc - SLOTS_B
            slot, side = 5 + pos // 2, pos % 2
        elif unit >= CHUNKS * e_loc:
            return wb.at[unit - CHUNKS * e_loc]
        elif unit >= SLOTS_B:
            slot, side = 1 + (unit - SLOTS_B) // 2, unit % 2
        else:
            return wb.at[unit]
        return wa.at[slot, pl.ds(0, ff), pl.ds(side * cw, cw)]

    def b_copy(unit):
        if unit < CHUNKS * e_loc:
            j, e = unit // e_loc, unit % e_loc
            src = ed_ref.at[e, :, pl.ds(j * cw, cw)]
        else:
            j, hf = (unit - CHUNKS * e_loc) // halves, (unit - CHUNKS * e_loc) % halves
            src = sd_ref.at[pl.ds(hf * ff, ff), pl.ds(j * cw, cw)]
        return pltpu.make_async_copy(src, b_place(unit), sem_b.at[unit])

    for unit in range(SLOTS_A):
        a_copy(unit).start()
    for unit in range(SLOTS_B):
        b_copy(unit).start()

    barrier = pltpu.get_barrier_semaphore()
    for dev in (up_dev, dn_dev, sib):
        pl.semaphore_signal(barrier, inc=1, device_id={'ep': dev}, device_id_type=MESH)
    pl.semaphore_wait(barrier, 3)

    def remote(src, dst, send, recv, dev):
        return pltpu.make_async_remote_copy(src_ref=src, dst_ref=dst, send_sem=send, recv_sem=recv,
                                            device_id={'ep': dev}, device_id_type=MESH)

    def h_hop(way, step, half):
        dev = up_dev if way == 0 else dn_dev
        origin = chip(-step if way == 0 else step)
        slot = slot_of(par, origin)
        cols = pl.ds(half * half_dim, half_dim)
        src = h_ref.at[:, cols] if step == 0 else hall.at[slot, :, cols]
        return remote(src, hall.at[slot, :, cols], ag_send.at[way, step, half], ag_recv.at[way, step, half], dev)

    def t_hop(way, step):
        dev = up_dev if way == 0 else dn_dev
        origin = chip(-step if way == 0 else step)
        slot = slot_of(par, origin)
        src = table_ref if step == 0 else gall.at[slot]
        return remote(src, gall.at[slot], tb_send.at[way, step], tb_recv.at[way, step], dev)

    def h_cross(k, origin):
        slot = slot_of(par, origin)
        src = h_ref if k == 0 else hall.at[slot]
        return remote(src, hall.at[slot], sib_send.at[k], sib_recv.at[k], sib)

    def t_cross(k, origin):
        slot = slot_of(par, origin)
        src = table_ref if k == 0 else gall.at[slot]
        return remote(src, gall.at[slot], ts_send.at[k], ts_recv.at[k], sib)

    t_steps = (far, far - 1)
    sent = []

    def go(copy):
        copy.start()
        sent.append(copy)
        return copy

    hops, thops = {}, {}
    for way in range(2):
        thops[way, 0] = go(t_hop(way, 0))
    for half in range(2):
        for way in range(2):
            hops[way, 0, half] = go(h_hop(way, 0, half))
    crossed = [go(t_cross(0, z)), go(h_cross(0, z))]
    hall[slot_of(par, z)] = h_ref[...]
    gall[slot_of(par, z)] = table_ref[...]
    for step in range(far):
        for way in range(2):
            if step < t_steps[way]:
                origin = chip(-(step + 1) if way == 0 else step + 1)
                thops[way, step].wait_recv()
                if step + 1 < t_steps[way]:
                    thops[way, step + 1] = go(t_hop(way, step + 1))
                crossed.append(go(t_cross(1 + 2 * step + way, origin)))
        for half in range(2):
            for way in range(2):
                if step < far - 1 or half == way:
                    hops[way, step, half].wait_recv()
                if step < far - 2 or (step == far - 2 and half == way):
                    hops[way, step + 1, half] = go(h_hop(way, step + 1, half))
        if step < far - 1:
            for way in range(2):
                crossed.append(go(h_cross(1 + 2 * step + way, chip(-(step + 1) if way == 0 else step + 1))))
    crossed.append(go(h_cross(2 * far - 1, chip(far))))
    for copy in crossed:
        copy.wait_recv()

    rowpat = rowpat_ref[...]
    row_exp, row_dev, row_slot = rowpat[:, 0:1], rowpat[:, 1:2], rowpat[:, 2:3]
    base = n_exp + e_loc * me
    lane = lax.broadcasted_iota(jnp.int32, (rows_all, LANES), 1)
    pick = jnp.where(lane == base + row_exp.astype(jnp.int32), 1.0, 0.0).astype(BF16)
    slots_by_row = lax.dot_general(pick, gall[...].reshape(n_ep * tok, LANES).astype(BF16), (((1,), (1,)), ((), ())),
                                   preferred_element_type=F32)
    tok_dev = (lax.broadcasted_iota(jnp.int32, (rows_all, n_ep * tok), 1) // tok).astype(F32)
    place = jnp.where((slots_by_row == row_slot) & (tok_dev == row_dev), 1.0, 0.0).astype(BF16)
    for start, width in wide_tiles(dim, 256):
        rows = hall[:, :, start:start + width].reshape(n_ep * tok, width)
        xg[:, :, start:start + width] = dot32(place, rows).astype(BF16).reshape(e_loc, rows_exp, width)

    colpat = colpat_ref[...]
    col_exp, col_chip, col_slot = colpat[0:1, :], colpat[1:2, :], colpat[2:3, :]
    g_own = gall[pl.ds(par * nz, nz)].reshape(nz * tok, LANES)
    part1 = g_own.astype(BF16)
    rest1 = g_own - part1.astype(F32)
    part2 = rest1.astype(BF16)
    part3 = (rest1 - part2.astype(F32)).astype(BF16)
    sub = lax.broadcasted_iota(jnp.int32, (LANES, rows_q), 0)
    tok_chip = (lax.broadcasted_iota(jnp.int32, (nz * tok, rows_q), 0) // tok).astype(F32)
    for q in range(2):
        ids = e_loc * (me if q == 0 else sib) + col_exp.astype(jnp.int32)
        sel_w = jnp.where(sub == ids, 1.0, 0.0).astype(BF16)
        sel_s = jnp.where(sub == n_exp + ids, 1.0, 0.0).astype(BF16)
        here = (dot32(part1, sel_s) == col_slot) & (tok_chip == col_chip)
        for i, part in enumerate((part1, part2, part3)):
            cmat[q, i] = jnp.where(here, dot32(part, sel_w), 0.0).astype(BF16)

    def swiglu_tile(x, slot_g, slot_u, start, width):
        gate = dot32(x, wa[slot_g, :, start:start + width])
        up = dot32(x, wa[slot_u, :, start:start + width])
        return (jax.nn.silu(gate) * up).astype(BF16)

    def expert_up(e, carry):
        slot_g = lax.rem(2 * e, SLOTS_A)
        slot_u = lax.rem(2 * e + 1, SLOTS_A)
        for unit, slot in ((2 * e, slot_g), (2 * e + 1, slot_u)):
            pltpu.make_async_copy(eg_ref.at[0], wa.at[slot], sem_a.at[unit]).wait()
        for start, width in wide_tiles(ff, 256):
            act[e, :, start:start + width] = swiglu_tile(xg[e], slot_g, slot_u, start, width)
        for e_st in range(e_loc):
            @pl.when(e == e_st)
            def _():
                if e_st == 0:
                    a_copy(SLOTS_A).start()
                    ahead = (4, 5)
                elif e_st < e_loc - 1:
                    ahead = range(4 * e_st + 2, 4 * e_st + 6)
                else:
                    ahead = (14, 15)
                for unit in ahead:
                    b_copy(unit).start()
                if e_st == e_loc - 1:
                    a_copy(2 * e_loc).start()
        return carry

    lax.fori_loop(0, e_loc, expert_up, 0)

    def reach(way, j):
        return far if (way + j) % 2 == 0 else nz - 1 - far

    def ring_copy(way, j, step):
        dev = up_dev if way == 0 else dn_dev
        ahead = reach(way, j) - step + 1
        dest = chip(ahead if way == 0 else -ahead)
        src = ct.at[j, dest] if step == 1 else ring.at[way, j, step - 2]
        return remote(src, ring.at[way, j, step - 1], rg_send.at[way, j, step - 1], rg_recv.at[way, j, step - 1], dev)

    rcopies = {}

    def combine(j):
        exch[j].wait_recv()
        own = ebuf[j, par].reshape(rows_q, cw)
        other = esib[j].reshape(rows_q, cw)
        for start, width in wide_tiles(cw, 256):
            total = dot32(cmat[0, 0], own[:, start:start + width]) + dot32(cmat[1, 0], other[:, start:start + width])
            for i in (1, 2):
                total += dot32(cmat[0, i], own[:, start:start + width]) + dot32(cmat[1, i], other[:, start:start + width])
            ct[j, :, :, start:start + width] = total.reshape(nz, tok, width)
        for way in range(2):
            rcopies[way, j, 1] = go(ring_copy(way, j, 1))

    def advance(j, step):
        for way in range(2):
            if step < reach(way, j):
                rcopies[way, j, step].wait_recv()
                ahead = reach(way, j) - step
                dest = chip(ahead if way == 0 else -ahead)
                ring[way, j, step - 1] += ct[j, dest]
                rcopies[way, j, step + 1] = go(ring_copy(way, j, step + 1))

    def finish(j):
        cols = slice(j * cw, (j + 1) * cw)
        total = resid_ref[:, cols].astype(F32) + sh_out[:, cols] + ct[j, z]
        for way in range(2):
            rcopies[way, j, reach(way, j)].wait_recv()
            total += ring[way, j, reach(way, j) - 1]
        out_ref[:, cols] = total.astype(BF16)

    exch = {}

    def down(j):
        for e in range(e_loc):
            b_copy(j * e_loc + e).wait()
        for e in range(e_loc):
            res = dot32(act[e], b_place(j * e_loc + e)[...]).astype(BF16)
            ebuf[j, 0, e] = res[:rows_par]
            ebuf[j, 1, e] = res[rows_par:]
        exch[j] = go(remote(ebuf.at[j, 1 - par], esib.at[j], ex_send.at[j], ex_recv.at[j], sib))
        shared = CHUNKS * e_loc
        if j == 1:
            a_copy(2 * e_loc + 1).start()
            a_copy(2 * e_loc + 2).start()
        elif j == 2:
            a_copy(2 * e_loc + 3).start()
            for pos in range(SLOTS_B):
                b_copy(shared + pos).start()
        elif j == 3:
            for pos in range(SLOTS_B, CHUNKS * halves):
                b_copy(shared + pos).start()

    def shared_up(hf, tile):
        unit = 2 * e_loc + 2 * hf
        start, width = wide_tiles(ff, 256)[tile]
        if tile == 0:
            a_copy(unit).wait()
            a_copy(unit + 1).wait()
        act_sh[hf, :, start:start + width] = swiglu_tile(h_ref[...], a_slot(unit), a_slot(unit + 1), start, width)

    def shared_down(j):
        total = jnp.zeros((tok, cw), F32)
        for hf in range(halves):
            unit = CHUNKS * e_loc + j * halves + hf
            b_copy(unit).wait()
            total += dot32(act_sh[hf], b_place(unit)[...])
        sh_out[:, j * cw:(j + 1) * cw] = total

    down(0)
    down(1)
    combine(0)
    down(2)
    combine(1)
    advance(0, 1)
    down(3)
    combine(2)
    advance(1, 1)
    advance(0, 2)
    combine(3)
    tiles = len(wide_tiles(ff, 256))
    pieces = [functools.partial(shared_up, hf, tile) for hf in range(halves) for tile in range(tiles)]
    pieces += [functools.partial(shared_down, j) for j in range(CHUNKS)]
    events = [(2, 1), (1, 2), (3, 1), (0, 3), (2, 2), (1, 3), (3, 2), (2, 3), (3, 3)]
    for i, event in enumerate(events):
        advance(*event)
        for piece in pieces[i * len(pieces) // len(events):(i + 1) * len(pieces) // len(events)]:
            piece()
    for j in range(CHUNKS):
        finish(j)
    for copy in sent:
        copy.wait_send()


def moe_call(n_ep, h_norm, table, resid, w_sg, w_su, w_sd, w_eg, w_eu, w_ed):
    nz = n_ep // 2
    tok, dim = h_norm.shape
    e_loc, _, ff = w_eg.shape
    n_exp = e_loc * n_ep
    halves = w_sg.shape[1] // ff
    far = nz // 2
    cw = dim // CHUNKS
    rows_par = nz * CAP
    rows_exp = 2 * rows_par
    rows_all = e_loc * rows_exp
    rows_q = e_loc * rows_par
    row = np.arange(rows_all)
    rowpat = np.zeros((rows_all, 8), np.float32)
    rowpat[:, 0] = row // rows_exp
    rowpat[:, 1] = (row % rows_exp) // CAP
    rowpat[:, 2] = row % CAP + 1
    col = np.arange(rows_q)
    colpat = np.zeros((8, rows_q), np.float32)
    colpat[0] = col // rows_par
    colpat[1] = (col % rows_par) // CAP
    colpat[2] = col % CAP + 1
    vmem = pl.BlockSpec(memory_space=pltpu.VMEM)
    hbm = pl.BlockSpec(memory_space=pl.ANY)
    dma = pltpu.SemaphoreType.DMA
    return pl.pallas_call(
        functools.partial(moe_kernel, n_ep, n_exp),
        out_shape=jax.ShapeDtypeStruct((tok, dim), BF16),
        in_specs=[vmem] * 5 + [hbm] * 6,
        out_specs=vmem,
        scratch_shapes=[
            pltpu.VMEM((n_ep, tok, dim), BF16),
            pltpu.VMEM((n_ep, tok, LANES), F32),
            pltpu.VMEM((e_loc, rows_exp, dim), BF16),
            pltpu.VMEM((e_loc, rows_exp, ff), BF16),
            pltpu.VMEM((halves, tok, ff), BF16),
            pltpu.VMEM((CHUNKS, 2, e_loc, rows_par, cw), BF16),
            pltpu.VMEM((CHUNKS, e_loc, rows_par, cw), BF16),
            pltpu.VMEM((2, 3, nz * tok, rows_q), BF16),
            pltpu.VMEM((CHUNKS, nz, tok, cw), F32),
            pltpu.VMEM((2, CHUNKS, far, tok, cw), F32),
            pltpu.VMEM((SLOTS_A, dim, ff), BF16),
            pltpu.VMEM((SLOTS_B, ff, cw), BF16),
            pltpu.VMEM((tok, dim), F32),
            dma((2 * (e_loc + halves),)), dma((CHUNKS * (e_loc + halves),)),
            dma((2, far, 2)), dma((2, far, 2)), dma((nz,)), dma((nz,)),
            dma((2, far)), dma((2, far)), dma((nz,)), dma((nz,)),
            dma((CHUNKS,)), dma((CHUNKS,)),
            dma((2, CHUNKS, far)), dma((2, CHUNKS, far)),
        ],
        compiler_params=pltpu.CompilerParams(collective_id=0, has_side_effects=True, vmem_limit_bytes=67000000),
        name='moe_ring',
    )(h_norm, table, resid, jnp.asarray(rowpat), jnp.asarray(colpat), w_sg, w_su, w_sd, w_eg, w_eu, w_ed)


def solution(mesh):
    n_ep = mesh.shape['ep']
    row_one = P(('dp', 'ep'))
    row_two = P(('dp', 'ep'), None)
    row_three = P(('dp', 'ep'), None, None)
    rep_one = P(None)
    rep_two = P(None, None)
    rep_three = P(None, None, None)
    exp_spec = P('ep', None, None)

    def local_step(tok_in, lat_cache, rope_cache, tok_pos, expert_ids, attn_gain, w_query, w_kvdown, w_ukey, w_uval, w_out, ffn_gain, w_router, sh_gate, sh_up, sh_down, ex_gate, ex_up, ex_down):
        resid_bf, h_norm, table, lat_out, rope_out = attn_call(tok_in, lat_cache, rope_cache, tok_pos, expert_ids, attn_gain, w_query, w_kvdown, w_ukey, w_uval, w_out, ffn_gain, w_router)
        out_hidden = moe_call(n_ep, h_norm, table, resid_bf, sh_gate, sh_up, sh_down, ex_gate, ex_up, ex_down)
        return out_hidden, lat_out, rope_out

    in_specs = (row_two, row_three, row_three, row_one, row_two, rep_one, rep_two, rep_two, rep_three, rep_three, rep_two, rep_one, rep_two, rep_two, rep_two, rep_two, exp_spec, exp_spec, exp_spec)
    out_specs = (row_two, row_three, row_three)
    return jax.shard_map(local_step, mesh=mesh, in_specs=in_specs, out_specs=out_specs, check_vma=False)
```

```python
import functools

import jax
import jax.numpy as jnp
import numpy as np
from jax import lax
from jax.experimental import pallas as pl
from jax.experimental.pallas import tpu as pltpu
from jax.sharding import PartitionSpec as P

ROUTE_SCALE = 2.827
ROPE_BASE = 10000.0
NORM_EPS = 1e-6
MESH = pl.DeviceIdType.MESH
F32 = jnp.float32
BF16 = jnp.bfloat16
CHUNKS = 4
SLOTS_A = 7
SLOTS_B = 4
CAP = 6
PARTS = 4
LANES = 128
GROUP = 4


def unit_norm(values):
    mean_sq = jnp.mean(jnp.square(values), axis=-1, keepdims=True)
    return values * lax.rsqrt(mean_sq + NORM_EPS)


def dot32(lhs, rhs):
    return jnp.dot(lhs, rhs, preferred_element_type=F32)


def wide_tiles(total, width):
    return [(start, min(width, total - start)) for start in range(0, total, width)]


def attn_kernel(pos_ref, x_ref, freq_ref, ids_ref, ag_ref, fg_ref, wq_ref, wkv_ref, uk_ref, uv_ref, wo_ref, wr_ref, lat_ref, rope_ref,
                res_ref, h_ref, table_ref, lat_out, rope_out,
                wq, wkv, uk, uv, wo, wr, lat, rope, q_lat, q_rope, o_lat, o_heads, score, prob, sem_q, sem_w, sem_c, sem_o):
    n_heads, nope, rank = uk_ref.shape
    tok, dim = x_ref.shape
    seq, rope_dim = rope_ref.shape[1:]
    half = rope_dim // 2
    head = nope + rope_dim
    n_exp = wr_ref.shape[0]
    blocks = n_heads // GROUP
    q_cols = GROUP * head

    def q_copy(blk):
        return pltpu.make_async_copy(wq_ref.at[:, pl.ds(blk * q_cols, q_cols)], wq.at[blk], sem_q.at[blk])

    kv_copy = pltpu.make_async_copy(wkv_ref, wkv, sem_w.at[0])
    uk_copy = pltpu.make_async_copy(uk_ref, uk, sem_w.at[1])
    uv_copy = pltpu.make_async_copy(uv_ref, uv, sem_w.at[2])
    wo_copy = pltpu.make_async_copy(wo_ref, wo, sem_w.at[3])
    wr_copy = pltpu.make_async_copy(wr_ref, wr, sem_w.at[4])
    lat_copy = pltpu.make_async_copy(lat_ref, lat, sem_c.at[0])
    rope_copy = pltpu.make_async_copy(rope_ref, rope, sem_c.at[1])
    kv_copy.start()
    q_copy(0).start()
    uk_copy.start()

    x = x_ref[...].astype(F32)
    x_norm = (unit_norm(x) * ag_ref[...].astype(F32).reshape(1, dim)).astype(BF16)
    tok_row = lax.broadcasted_iota(jnp.int32, (tok, half), 0)
    pos = jnp.zeros((tok, half), jnp.int32)
    for t in range(tok):
        pos = jnp.where(tok_row == t, pos_ref[t], pos)
    angle = pos.astype(F32) * freq_ref[...]
    cos, sin = jnp.cos(angle), jnp.sin(angle)
    across = (((1,), (1,)), ((), ()))

    def rotate(first, second):
        return jnp.concatenate([first * cos - second * sin, second * cos + first * sin], axis=1)

    kv_copy.wait()
    q_copy(1).start()
    if blocks > 2:
        q_copy(2).start()
    kv = lax.dot_general(x_norm, wkv[...], across, preferred_element_type=F32)
    lat_new = unit_norm(kv[:, :rank]).astype(BF16).astype(F32)
    rope_new = rotate(kv[:, rank:rank + half], kv[:, rank + half:]).astype(BF16).astype(F32)

    def spread(ref, n, val):
        for c in range(val.shape[1] // LANES):
            ref[c, pl.ds(n, tok, stride=n_heads), :] = val[:, c * LANES:(c + 1) * LANES]

    uk_copy.wait()
    for blk in range(blocks):
        q_copy(blk).wait()
        if blk == 0:
            lat_copy.start()
            rope_copy.start()
            if blocks > 3:
                q_copy(3).start()
        elif blk == 1:
            uv_copy.start()
            wr_copy.start()
        if blk == blocks - 2:
            wo_copy.start()
        q = dot32(x_norm, wq[blk]).astype(BF16)
        for i in range(GROUP):
            n = blk * GROUP + i
            at = i * head
            q_n = dot32(q[:, at:at + nope], uk[n]).astype(BF16).astype(F32)
            spread(q_lat, n, q_n)
            q_r = q[:, at + nope:at + head].astype(F32)
            q_r = rotate(q_r[:, :half], q_r[:, half:]).astype(BF16).astype(F32)
            spread(q_rope, n, jnp.concatenate([q_r, jnp.zeros((tok, LANES - rope_dim), F32)], axis=1))
    lat_copy.wait()
    rope_copy.wait()
    rows, keys = GROUP * n_heads, GROUP * seq
    key = lax.broadcasted_iota(jnp.int32, (rows, keys), 1)
    same = (key // seq) == (lax.broadcasted_iota(jnp.int32, (rows, keys), 0) // n_heads)
    key_tok, key_seq = key // seq, lax.rem(key, seq)
    groups = tok // GROUP

    def grouped(g):
        lat_g = lat[g * GROUP:(g + 1) * GROUP].reshape(keys, rank)
        rope_g = rope[g * GROUP:(g + 1) * GROUP].reshape(keys, rope_dim)
        return slice(g * rows, (g + 1) * rows), lat_g, rope_g

    lat_row = lax.broadcasted_iota(jnp.int32, (seq, rank), 0)
    rope_row = lax.broadcasted_iota(jnp.int32, (seq, rope_dim), 0)
    for t in range(tok):
        lat[t] = jnp.where(lat_row == pos_ref[t], lat_new[t:t + 1], lat[t].astype(F32)).astype(BF16)
        rope[t] = jnp.where(rope_row == pos_ref[t], rope_new[t:t + 1], rope[t].astype(F32)).astype(BF16)
    lat_back = pltpu.make_async_copy(lat, lat_out, sem_o.at[0])
    rope_back = pltpu.make_async_copy(rope, rope_out, sem_o.at[1])
    for g in range(groups):
        sl, lat_g, rope_g = grouped(g)
        q_g = jnp.concatenate([q_lat[c, sl] for c in range(rank // LANES)], axis=1).astype(BF16)
        score[g] = (lax.dot_general(q_g, lat_g, across, preferred_element_type=F32)
                    + lax.dot_general(q_rope[0, sl, :rope_dim].astype(BF16), rope_g, across, preferred_element_type=F32))
    for g in range(groups):
        last = jnp.full((rows, keys), pos_ref[g * GROUP], jnp.int32)
        for i in range(1, GROUP):
            last = jnp.where(key_tok == i, pos_ref[g * GROUP + i], last)
        masked = jnp.where(same & (key_seq <= last), score[g] * head ** -0.5, -jnp.inf)
        expd = jnp.exp(masked - jnp.max(masked, axis=1, keepdims=True))
        prob[g] = (expd / jnp.sum(expd, axis=1, keepdims=True)).astype(BF16)
    for g in range(groups):
        sl, lat_g, _ = grouped(g)
        o_g = dot32(prob[g], lat_g).astype(BF16).astype(F32)
        for c in range(rank // LANES):
            o_lat[c, sl] = o_g[:, c * LANES:(c + 1) * LANES]
    lat_back.start()
    rope_back.start()

    uv_copy.wait()
    for n in range(n_heads):
        o_n = jnp.concatenate([o_lat[c, pl.ds(n, tok, stride=n_heads), :] for c in range(rank // LANES)], axis=1).astype(BF16)
        o_heads[:, n * uv.shape[2]:(n + 1) * uv.shape[2]] = dot32(o_n, uv[n]).astype(BF16)
    wr_copy.wait()
    wo_copy.wait()
    for start, width in wide_tiles(dim, 512):
        attn = dot32(o_heads[...], wo[:, start:start + width])
        res_ref[:, start:start + width] = (x[:, start:start + width] + attn).astype(BF16)
    h = (unit_norm(res_ref[...].astype(F32)) * fg_ref[...].astype(F32).reshape(1, dim)).astype(BF16)
    h_ref[...] = h

    gate = jax.nn.sigmoid(lax.dot_general(h, wr[...], across, preferred_element_type=F32))
    exp_row = lax.broadcasted_iota(jnp.int32, (n_exp, tok), 0)
    listed_t = jnp.zeros((n_exp, tok), F32)
    for i in range(ids_ref.shape[0]):
        listed_t = listed_t + jnp.where(exp_row == ids_ref[i:i + 1, :], 1.0, 0.0)
    listed_t = listed_t.astype(BF16)
    row, col = lax.broadcasted_iota(jnp.int32, (tok, tok), 0), lax.broadcasted_iota(jnp.int32, (tok, tok), 1)
    listed = lax.dot_general(jnp.where(row == col, 1.0, 0.0).astype(BF16), listed_t, across, preferred_element_type=F32)
    slots = lax.dot_general(jnp.where(row >= col, 1.0, 0.0).astype(BF16), listed_t, across, preferred_element_type=F32) * listed
    chosen = gate * listed
    table_ref[:, :n_exp] = ROUTE_SCALE * chosen / jnp.sum(chosen, axis=1, keepdims=True)
    table_ref[:, n_exp:] = slots
    lat_back.wait()
    rope_back.wait()


def attn_call(tok_in, lat_cache, rope_cache, tok_pos, expert_ids, attn_gain, w_query, w_kvdown, w_ukey, w_uval, w_out, ffn_gain, w_router):
    tok, dim = tok_in.shape
    n_heads, nope, rank = w_ukey.shape
    seq, rope_dim = rope_cache.shape[1:]
    n_exp = w_router.shape[1]
    blocks = n_heads // GROUP
    inv_freq = ROPE_BASE ** (-(2.0 * np.arange(rope_dim // 2)) / rope_dim)
    freq = jnp.asarray(inv_freq[None, :].astype(np.float32))
    vmem = pl.BlockSpec(memory_space=pltpu.VMEM)
    hbm = pl.BlockSpec(memory_space=pl.ANY)
    dma = pltpu.SemaphoreType.DMA
    return pl.pallas_call(
        attn_kernel,
        out_shape=[
            jax.ShapeDtypeStruct((tok, dim), BF16),
            jax.ShapeDtypeStruct((tok, dim), BF16),
            jax.ShapeDtypeStruct((tok, 2 * n_exp), F32),
            jax.ShapeDtypeStruct(lat_cache.shape, BF16),
            jax.ShapeDtypeStruct(rope_cache.shape, BF16),
        ],
        in_specs=[pl.BlockSpec(memory_space=pltpu.SMEM)] + [vmem] * 5 + [hbm] * 8,
        out_specs=[vmem, vmem, vmem, hbm, hbm],
        scratch_shapes=[
            pltpu.VMEM((blocks, dim, w_query.shape[1] // blocks), BF16),
            pltpu.VMEM(w_kvdown.shape[::-1], BF16),
            pltpu.VMEM(w_ukey.shape, BF16),
            pltpu.VMEM(w_uval.shape, BF16),
            pltpu.VMEM(w_out.shape, BF16),
            pltpu.VMEM(w_router.shape[::-1], BF16),
            pltpu.VMEM(lat_cache.shape, BF16),
            pltpu.VMEM(rope_cache.shape, BF16),
            pltpu.VMEM((rank // LANES, tok * n_heads, LANES), F32),
            pltpu.VMEM((1, tok * n_heads, LANES), F32),
            pltpu.VMEM((rank // LANES, tok * n_heads, LANES), F32),
            pltpu.VMEM((tok, w_out.shape[0]), BF16),
            pltpu.VMEM((tok // GROUP, GROUP * n_heads, GROUP * seq), F32),
            pltpu.VMEM((tok // GROUP, GROUP * n_heads, GROUP * seq), BF16),
            dma((blocks,)), dma((5,)), dma((2,)), dma((2,)),
        ],
        compiler_params=pltpu.CompilerParams(vmem_limit_bytes=60000000),
        name='latent_attention',
    )(tok_pos, tok_in, freq, expert_ids.T, attn_gain, ffn_gain, w_query, w_kvdown.T, w_ukey, w_uval, w_out, w_router.T, lat_cache, rope_cache)


def moe_kernel(n_ep, n_exp, h_ref, table_ref, resid_ref, rowpat_ref, colpat_ref,
               sg_ref, su_ref, sd_ref, eg_ref, eu_ref, ed_ref, out_ref,
               hall, gall, xg, act, act_sh, ebuf, esib, cmat, ct, ring, wa, wb, sh_out,
               sem_a, sem_b, ag_send, ag_recv, sib_send, sib_recv, tb_send, tb_recv, ts_send, ts_recv,
               ex_send, ex_recv, rg_send, rg_recv):
    nz = n_ep // 2
    far = nz // 2
    tok, dim = h_ref.shape
    e_loc, _, ff = eg_ref.shape
    halves = sg_ref.shape[1] // ff
    rows_par = nz * CAP
    rows_exp = 2 * rows_par
    rows_all = e_loc * rows_exp
    rows_q = e_loc * rows_par
    cw = dim // CHUNKS
    part_dim = dim // PARTS

    me = lax.axis_index('ep')
    z = me // 2
    par = lax.rem(me, 2)
    sib = me + 1 - 2 * par
    up_dev = lax.rem(z + 1, nz) * 2 + par
    dn_dev = lax.rem(z + nz - 1, nz) * 2 + par

    def chip(step):
        return lax.rem(z + step + 2 * nz, nz)

    def slot_of(p, zz):
        return p * nz + zz

    def a_slot(unit):
        return unit % SLOTS_A if unit < 2 * e_loc else unit - 2 * e_loc

    def a_copy(unit):
        slot = a_slot(unit)
        if unit < 2 * e_loc:
            src = (eg_ref if unit % 2 == 0 else eu_ref).at[unit // 2]
        else:
            hf = (unit - 2 * e_loc) // 2
            src = (sg_ref if unit % 2 == 0 else su_ref).at[:, pl.ds(hf * ff, ff)]
        return pltpu.make_async_copy(src, wa.at[slot], sem_a.at[unit])

    def b_place(unit):
        if unit >= CHUNKS * e_loc + SLOTS_B:
            pos = unit - CHUNKS * e_loc - SLOTS_B
            slot, side = 5 + pos // 2, pos % 2
        elif unit >= CHUNKS * e_loc:
            return wb.at[unit - CHUNKS * e_loc]
        elif unit >= SLOTS_B:
            slot, side = 1 + (unit - SLOTS_B) // 2, unit % 2
        else:
            return wb.at[unit]
        return wa.at[slot, pl.ds(0, ff), pl.ds(side * cw, cw)]

    def b_copy(unit):
        if unit < CHUNKS * e_loc:
            j, e = unit // e_loc, unit % e_loc
            src = ed_ref.at[e, :, pl.ds(j * cw, cw)]
        else:
            j, hf = (unit - CHUNKS * e_loc) // halves, (unit - CHUNKS * e_loc) % halves
            src = sd_ref.at[pl.ds(hf * ff, ff), pl.ds(j * cw, cw)]
        return pltpu.make_async_copy(src, b_place(unit), sem_b.at[unit])

    for unit in range(SLOTS_A):
        a_copy(unit).start()
    for unit in range(SLOTS_B):
        b_copy(unit).start()

    barrier = pltpu.get_barrier_semaphore()
    for dev in (up_dev, dn_dev, sib):
        pl.semaphore_signal(barrier, inc=1, device_id={'ep': dev}, device_id_type=MESH)
    pl.semaphore_wait(barrier, 3)

    def remote(src, dst, send, recv, dev):
        return pltpu.make_async_remote_copy(src_ref=src, dst_ref=dst, send_sem=send, recv_sem=recv,
                                            device_id={'ep': dev}, device_id_type=MESH)

    def h_hop(way, step, part):
        dev = up_dev if way == 0 else dn_dev
        origin = chip(-step if way == 0 else step)
        slot = slot_of(par, origin)
        cols = pl.ds(part * part_dim, part_dim)
        src = h_ref.at[:, cols] if step == 0 else hall.at[slot, :, cols]
        return remote(src, hall.at[slot, :, cols], ag_send.at[way, step, part], ag_recv.at[way, step, part], dev)

    def t_hop(way, step):
        dev = up_dev if way == 0 else dn_dev
        origin = chip(-step if way == 0 else step)
        slot = slot_of(par, origin)
        src = table_ref if step == 0 else gall.at[slot]
        return remote(src, gall.at[slot], tb_send.at[way, step], tb_recv.at[way, step], dev)

    def h_cross(k, origin):
        slot = slot_of(par, origin)
        src = h_ref if k == 0 else hall.at[slot]
        return remote(src, hall.at[slot], sib_send.at[k], sib_recv.at[k], sib)

    def t_cross(k, origin):
        slot = slot_of(par, origin)
        src = table_ref if k == 0 else gall.at[slot]
        return remote(src, gall.at[slot], ts_send.at[k], ts_recv.at[k], sib)

    t_steps = (far, far - 1)

    def place_rows():
        rowpat = rowpat_ref[...]
        row_exp, row_dev, row_slot = rowpat[:, 0:1], rowpat[:, 1:2], rowpat[:, 2:3]
        base = n_exp + e_loc * me
        lane = lax.broadcasted_iota(jnp.int32, (rows_all, LANES), 1)
        pick = jnp.where(lane == base + row_exp.astype(jnp.int32), 1.0, 0.0).astype(BF16)
        slots_by_row = lax.dot_general(pick, gall[...].reshape(n_ep * tok, LANES).astype(BF16), (((1,), (1,)), ((), ())),
                                       preferred_element_type=F32)
        tok_dev = (lax.broadcasted_iota(jnp.int32, (rows_all, n_ep * tok), 1) // tok).astype(F32)
        return jnp.where((slots_by_row == row_slot) & (tok_dev == row_dev), 1.0, 0.0).astype(BF16)

    def combine_weights():
        colpat = colpat_ref[...]
        col_exp, col_chip, col_slot = colpat[0:1, :], colpat[1:2, :], colpat[2:3, :]
        g_own = gall[pl.ds(par * nz, nz)].reshape(nz * tok, LANES)
        part1 = g_own.astype(BF16)
        rest1 = g_own - part1.astype(F32)
        part2 = rest1.astype(BF16)
        part3 = (rest1 - part2.astype(F32)).astype(BF16)
        sub = lax.broadcasted_iota(jnp.int32, (LANES, rows_q), 0)
        tok_chip = (lax.broadcasted_iota(jnp.int32, (nz * tok, rows_q), 0) // tok).astype(F32)
        for q in range(2):
            ids = e_loc * (me if q == 0 else sib) + col_exp.astype(jnp.int32)
            sel_w = jnp.where(sub == ids, 1.0, 0.0).astype(BF16)
            sel_s = jnp.where(sub == n_exp + ids, 1.0, 0.0).astype(BF16)
            here = (dot32(part1, sel_s) == col_slot) & (tok_chip == col_chip)
            for i, part in enumerate((part1, part2, part3)):
                cmat[q, i] = jnp.where(here, dot32(part, sel_w), 0.0).astype(BF16)
    sent = []

    def go(copy):
        copy.start()
        sent.append(copy)
        return copy

    hops, thops = {}, {}

    def goes(way, step, part):
        return step < far - 1 or part // (PARTS // 2) == way

    for way in range(2):
        thops[way, 0] = go(t_hop(way, 0))
    for part in range(PARTS):
        for way in range(2):
            hops[way, 0, part] = go(h_hop(way, 0, part))
    t_crossed, h_crossed = [go(t_cross(0, z))], [go(h_cross(0, z))]
    hall[slot_of(par, z)] = h_ref[...]
    gall[slot_of(par, z)] = table_ref[...]
    for step in range(far):
        for way in range(2):
            if step < t_steps[way]:
                origin = chip(-(step + 1) if way == 0 else step + 1)
                thops[way, step].wait_recv()
                if step + 1 < t_steps[way]:
                    thops[way, step + 1] = go(t_hop(way, step + 1))
                t_crossed.append(go(t_cross(1 + 2 * step + way, origin)))
        if step == far - 1:
            for copy in t_crossed:
                copy.wait_recv()
            place = place_rows()
            combine_weights()
        for part in range(PARTS):
            for way in range(2):
                if goes(way, step, part):
                    hops[way, step, part].wait_recv()
                    if step + 1 < far and goes(way, step + 1, part):
                        hops[way, step + 1, part] = go(h_hop(way, step + 1, part))
        if step < far - 1:
            for way in range(2):
                h_crossed.append(go(h_cross(1 + 2 * step + way, chip(-(step + 1) if way == 0 else step + 1))))
    h_crossed.append(go(h_cross(2 * far - 1, chip(far))))
    for copy in h_crossed:
        copy.wait_recv()
    for start, width in wide_tiles(dim, 256):
        rows = hall[:, :, start:start + width].reshape(n_ep * tok, width)
        xg[:, :, start:start + width] = dot32(place, rows).astype(BF16).reshape(e_loc, rows_exp, width)

    def swiglu_tile(x, slot_g, slot_u, start, width):
        gate = dot32(x, wa[slot_g, :, start:start + width])
        up = dot32(x, wa[slot_u, :, start:start + width])
        return (jax.nn.silu(gate) * up).astype(BF16)

    def expert_up(e, carry):
        slot_g = lax.rem(2 * e, SLOTS_A)
        slot_u = lax.rem(2 * e + 1, SLOTS_A)
        for unit, slot in ((2 * e, slot_g), (2 * e + 1, slot_u)):
            pltpu.make_async_copy(eg_ref.at[0], wa.at[slot], sem_a.at[unit]).wait()
        for start, width in wide_tiles(ff, 256):
            act[e, :, start:start + width] = swiglu_tile(xg[e], slot_g, slot_u, start, width)
        for e_st in range(e_loc):
            @pl.when(e == e_st)
            def _():
                if e_st == 0:
                    a_copy(SLOTS_A).start()
                    ahead = (4, 5)
                elif e_st < e_loc - 1:
                    ahead = range(4 * e_st + 2, 4 * e_st + 6)
                else:
                    ahead = (14, 15)
                for unit in ahead:
                    b_copy(unit).start()
                if e_st == e_loc - 1:
                    a_copy(2 * e_loc).start()
        return carry

    lax.fori_loop(0, e_loc, expert_up, 0)

    def reach(way, j):
        return far if (way + j) % 2 == 0 else nz - 1 - far

    def ring_copy(way, j, step):
        dev = up_dev if way == 0 else dn_dev
        ahead = reach(way, j) - step + 1
        dest = chip(ahead if way == 0 else -ahead)
        src = ct.at[j, dest] if step == 1 else ring.at[way, j, step - 2]
        return remote(src, ring.at[way, j, step - 1], rg_send.at[way, j, step - 1], rg_recv.at[way, j, step - 1], dev)

    rcopies = {}

    def combine(j):
        exch[j].wait_recv()
        own = ebuf[j, par].reshape(rows_q, cw)
        other = esib[j].reshape(rows_q, cw)
        for start, width in wide_tiles(cw, 256):
            total = dot32(cmat[0, 0], own[:, start:start + width]) + dot32(cmat[1, 0], other[:, start:start + width])
            for i in (1, 2):
                total += dot32(cmat[0, i], own[:, start:start + width]) + dot32(cmat[1, i], other[:, start:start + width])
            ct[j, :, :, start:start + width] = total.reshape(nz, tok, width)
        for way in range(2):
            rcopies[way, j, 1] = go(ring_copy(way, j, 1))

    def advance(j, step):
        for way in range(2):
            if step < reach(way, j):
                rcopies[way, j, step].wait_recv()
                ahead = reach(way, j) - step
                dest = chip(ahead if way == 0 else -ahead)
                ring[way, j, step - 1] += ct[j, dest]
                rcopies[way, j, step + 1] = go(ring_copy(way, j, step + 1))

    def finish(j):
        cols = slice(j * cw, (j + 1) * cw)
        total = resid_ref[:, cols].astype(F32) + sh_out[:, cols] + ct[j, z]
        for way in range(2):
            rcopies[way, j, reach(way, j)].wait_recv()
            total += ring[way, j, reach(way, j) - 1]
        out_ref[:, cols] = total.astype(BF16)

    exch = {}

    def down(j):
        for e in range(e_loc):
            b_copy(j * e_loc + e).wait()
        for e in range(e_loc):
            res = dot32(act[e], b_place(j * e_loc + e)[...]).astype(BF16)
            ebuf[j, 0, e] = res[:rows_par]
            ebuf[j, 1, e] = res[rows_par:]
        exch[j] = go(remote(ebuf.at[j, 1 - par], esib.at[j], ex_send.at[j], ex_recv.at[j], sib))
        shared = CHUNKS * e_loc
        if j == 1:
            a_copy(2 * e_loc + 1).start()
            a_copy(2 * e_loc + 2).start()
        elif j == 2:
            a_copy(2 * e_loc + 3).start()
            for pos in range(SLOTS_B):
                b_copy(shared + pos).start()
        elif j == 3:
            for pos in range(SLOTS_B, CHUNKS * halves):
                b_copy(shared + pos).start()

    def shared_up(hf, tile):
        unit = 2 * e_loc + 2 * hf
        start, width = wide_tiles(ff, 256)[tile]
        if tile == 0:
            a_copy(unit).wait()
            a_copy(unit + 1).wait()
        act_sh[hf, :, start:start + width] = swiglu_tile(h_ref[...], a_slot(unit), a_slot(unit + 1), start, width)

    def shared_down(j):
        total = jnp.zeros((tok, cw), F32)
        for hf in range(halves):
            unit = CHUNKS * e_loc + j * halves + hf
            b_copy(unit).wait()
            total += dot32(act_sh[hf], b_place(unit)[...])
        sh_out[:, j * cw:(j + 1) * cw] = total

    down(0)
    down(1)
    combine(0)
    down(2)
    combine(1)
    down(3)
    combine(2)
    combine(3)
    tiles = len(wide_tiles(ff, 256))
    pieces = [functools.partial(shared_up, hf, tile) for hf in range(halves) for tile in range(tiles)]
    pieces += [functools.partial(shared_down, j) for j in range(CHUNKS)]
    events = [(j, step) for step in range(1, far) for j in range(CHUNKS)]
    for i, event in enumerate(events):
        advance(*event)
        for piece in pieces[i * len(pieces) // len(events):(i + 1) * len(pieces) // len(events)]:
            piece()
    for j in range(CHUNKS):
        finish(j)
    for copy in sent:
        copy.wait_send()


def moe_call(n_ep, h_norm, table, resid, w_sg, w_su, w_sd, w_eg, w_eu, w_ed):
    nz = n_ep // 2
    tok, dim = h_norm.shape
    e_loc, _, ff = w_eg.shape
    n_exp = e_loc * n_ep
    halves = w_sg.shape[1] // ff
    far = nz // 2
    cw = dim // CHUNKS
    rows_par = nz * CAP
    rows_exp = 2 * rows_par
    rows_all = e_loc * rows_exp
    rows_q = e_loc * rows_par
    row = np.arange(rows_all)
    rowpat = np.zeros((rows_all, 8), np.float32)
    rowpat[:, 0] = row // rows_exp
    rowpat[:, 1] = (row % rows_exp) // CAP
    rowpat[:, 2] = row % CAP + 1
    col = np.arange(rows_q)
    colpat = np.zeros((8, rows_q), np.float32)
    colpat[0] = col // rows_par
    colpat[1] = (col % rows_par) // CAP
    colpat[2] = col % CAP + 1
    vmem = pl.BlockSpec(memory_space=pltpu.VMEM)
    hbm = pl.BlockSpec(memory_space=pl.ANY)
    dma = pltpu.SemaphoreType.DMA
    return pl.pallas_call(
        functools.partial(moe_kernel, n_ep, n_exp),
        out_shape=jax.ShapeDtypeStruct((tok, dim), BF16),
        in_specs=[vmem] * 5 + [hbm] * 6,
        out_specs=vmem,
        scratch_shapes=[
            pltpu.VMEM((n_ep, tok, dim), BF16),
            pltpu.VMEM((n_ep, tok, LANES), F32),
            pltpu.VMEM((e_loc, rows_exp, dim), BF16),
            pltpu.VMEM((e_loc, rows_exp, ff), BF16),
            pltpu.VMEM((halves, tok, ff), BF16),
            pltpu.VMEM((CHUNKS, 2, e_loc, rows_par, cw), BF16),
            pltpu.VMEM((CHUNKS, e_loc, rows_par, cw), BF16),
            pltpu.VMEM((2, 3, nz * tok, rows_q), BF16),
            pltpu.VMEM((CHUNKS, nz, tok, cw), F32),
            pltpu.VMEM((2, CHUNKS, far, tok, cw), F32),
            pltpu.VMEM((SLOTS_A, dim, ff), BF16),
            pltpu.VMEM((SLOTS_B, ff, cw), BF16),
            pltpu.VMEM((tok, dim), F32),
            dma((2 * (e_loc + halves),)), dma((CHUNKS * (e_loc + halves),)),
            dma((2, far, PARTS)), dma((2, far, PARTS)), dma((nz,)), dma((nz,)),
            dma((2, far)), dma((2, far)), dma((nz,)), dma((nz,)),
            dma((CHUNKS,)), dma((CHUNKS,)),
            dma((2, CHUNKS, far)), dma((2, CHUNKS, far)),
        ],
        compiler_params=pltpu.CompilerParams(collective_id=0, has_side_effects=True, vmem_limit_bytes=67000000),
        name='moe_ring',
    )(h_norm, table, resid, jnp.asarray(rowpat), jnp.asarray(colpat), w_sg, w_su, w_sd, w_eg, w_eu, w_ed)


def solution(mesh):
    n_ep = mesh.shape['ep']
    row_one = P(('dp', 'ep'))
    row_two = P(('dp', 'ep'), None)
    row_three = P(('dp', 'ep'), None, None)
    rep_one = P(None)
    rep_two = P(None, None)
    rep_three = P(None, None, None)
    exp_spec = P('ep', None, None)

    def local_step(tok_in, lat_cache, rope_cache, tok_pos, expert_ids, attn_gain, w_query, w_kvdown, w_ukey, w_uval, w_out, ffn_gain, w_router, sh_gate, sh_up, sh_down, ex_gate, ex_up, ex_down):
        resid_bf, h_norm, table, lat_out, rope_out = attn_call(tok_in, lat_cache, rope_cache, tok_pos, expert_ids, attn_gain, w_query, w_kvdown, w_ukey, w_uval, w_out, ffn_gain, w_router)
        out_hidden = moe_call(n_ep, h_norm, table, resid_bf, sh_gate, sh_up, sh_down, ex_gate, ex_up, ex_down)
        return out_hidden, lat_out, rope_out

    in_specs = (row_two, row_three, row_three, row_one, row_two, rep_one, rep_two, rep_two, rep_three, rep_three, rep_two, rep_one, rep_two, rep_two, rep_two, rep_two, exp_spec, exp_spec, exp_spec)
    out_specs = (row_two, row_three, row_three)
    return jax.shard_map(local_step, mesh=mesh, in_specs=in_specs, out_specs=out_specs, check_vma=False)
```

```python
import functools

import jax
import jax.numpy as jnp
import numpy as np
from jax import lax
from jax.experimental import pallas as pl
from jax.experimental.pallas import tpu as pltpu
from jax.sharding import PartitionSpec as P

ROUTE_SCALE = 2.827
ROPE_BASE = 10000.0
NORM_EPS = 1e-6
MESH = pl.DeviceIdType.MESH
F32 = jnp.float32
BF16 = jnp.bfloat16
CHUNKS = 4
RINGS = 8
TILE = 256
SLOTS_A = 7
SLOTS_B = 4
CAP = 6
PARTS = 4
LANES = 128
GROUP = 4


def unit_norm(values):
    mean_sq = jnp.mean(jnp.square(values), axis=-1, keepdims=True)
    return values * lax.rsqrt(mean_sq + NORM_EPS)


def dot32(lhs, rhs):
    return jnp.dot(lhs, rhs, preferred_element_type=F32)


def wide_tiles(total, width):
    return [(start, min(width, total - start)) for start in range(0, total, width)]


def attn_kernel(pos_ref, x_ref, freq_ref, ids_ref, ag_ref, fg_ref, wq_ref, wkv_ref, uk_ref, uv_ref, wo_ref, wr_ref, lat_ref, rope_ref,
                res_ref, h_ref, table_ref, lat_out, rope_out,
                wq, wkv, uk, uv, wo, wr, lat, rope, q_lat, q_rope, o_lat, o_heads, score, prob, sem_q, sem_w, sem_c, sem_o):
    n_heads, nope, rank = uk_ref.shape
    tok, dim = x_ref.shape
    seq, rope_dim = rope_ref.shape[1:]
    half = rope_dim // 2
    head = nope + rope_dim
    n_exp = wr_ref.shape[0]
    blocks = n_heads // GROUP
    q_cols = GROUP * head

    def q_copy(blk):
        return pltpu.make_async_copy(wq_ref.at[:, pl.ds(blk * q_cols, q_cols)], wq.at[blk], sem_q.at[blk])

    kv_copy = pltpu.make_async_copy(wkv_ref, wkv, sem_w.at[0])
    uk_copy = pltpu.make_async_copy(uk_ref, uk, sem_w.at[1])
    uv_copy = pltpu.make_async_copy(uv_ref, uv, sem_w.at[2])
    wo_copies = [pltpu.make_async_copy(wo_ref.at[:, pl.ds(i * dim // 2, dim // 2)], wo.at[i], sem_w.at[3 + i]) for i in range(2)]
    wr_copy = pltpu.make_async_copy(wr_ref, wr, sem_w.at[5])
    lat_copy = pltpu.make_async_copy(lat_ref, lat, sem_c.at[0])
    rope_copy = pltpu.make_async_copy(rope_ref, rope, sem_c.at[1])
    kv_copy.start()
    q_copy(0).start()
    uk_copy.start()
    q_copy(1).start()

    x = x_ref[...].astype(F32)
    x_norm = (unit_norm(x) * ag_ref[...].astype(F32).reshape(1, dim)).astype(BF16)
    tok_row = lax.broadcasted_iota(jnp.int32, (tok, half), 0)
    pos = jnp.zeros((tok, half), jnp.int32)
    for t in range(tok):
        pos = jnp.where(tok_row == t, pos_ref[t], pos)
    angle = pos.astype(F32) * freq_ref[...]
    cos, sin = jnp.cos(angle), jnp.sin(angle)
    across = (((1,), (1,)), ((), ()))

    def rotate(first, second):
        return jnp.concatenate([first * cos - second * sin, second * cos + first * sin], axis=1)

    kv_copy.wait()
    for blk in range(2, blocks):
        q_copy(blk).start()
    kv = lax.dot_general(x_norm, wkv[...], across, preferred_element_type=F32)
    lat_new = unit_norm(kv[:, :rank]).astype(BF16).astype(F32)
    rope_new = rotate(kv[:, rank:rank + half], kv[:, rank + half:]).astype(BF16).astype(F32)

    def spread(ref, n, val):
        for c in range(val.shape[1] // LANES):
            ref[c, pl.ds(n, tok, stride=n_heads), :] = val[:, c * LANES:(c + 1) * LANES]

    uk_copy.wait()
    for blk in range(blocks):
        q_copy(blk).wait()
        if blk == 0:
            lat_copy.start()
            rope_copy.start()
            uv_copy.start()
        elif blk == 1:
            wr_copy.start()
            for copy in wo_copies:
                copy.start()
        q = dot32(x_norm, wq[blk]).astype(BF16)
        for i in range(GROUP):
            n = blk * GROUP + i
            at = i * head
            q_n = dot32(q[:, at:at + nope], uk[n]).astype(BF16).astype(F32)
            spread(q_lat, n, q_n)
            q_r = q[:, at + nope:at + head].astype(F32)
            q_r = rotate(q_r[:, :half], q_r[:, half:]).astype(BF16).astype(F32)
            spread(q_rope, n, jnp.concatenate([q_r, jnp.zeros((tok, LANES - rope_dim), F32)], axis=1))
    lat_copy.wait()
    rope_copy.wait()
    rows, keys = GROUP * n_heads, GROUP * seq
    key = lax.broadcasted_iota(jnp.int32, (rows, keys), 1)
    same = (key // seq) == (lax.broadcasted_iota(jnp.int32, (rows, keys), 0) // n_heads)
    key_tok, key_seq = key // seq, lax.rem(key, seq)
    groups = tok // GROUP

    def grouped(g):
        lat_g = lat[g * GROUP:(g + 1) * GROUP].reshape(keys, rank)
        rope_g = rope[g * GROUP:(g + 1) * GROUP].reshape(keys, rope_dim)
        return slice(g * rows, (g + 1) * rows), lat_g, rope_g

    lat_row = lax.broadcasted_iota(jnp.int32, (seq, rank), 0)
    rope_row = lax.broadcasted_iota(jnp.int32, (seq, rope_dim), 0)
    for t in range(tok):
        lat[t] = jnp.where(lat_row == pos_ref[t], lat_new[t:t + 1], lat[t].astype(F32)).astype(BF16)
        rope[t] = jnp.where(rope_row == pos_ref[t], rope_new[t:t + 1], rope[t].astype(F32)).astype(BF16)
    lat_back = pltpu.make_async_copy(lat, lat_out, sem_o.at[0])
    rope_back = pltpu.make_async_copy(rope, rope_out, sem_o.at[1])
    for g in range(groups):
        sl, lat_g, rope_g = grouped(g)
        q_g = jnp.concatenate([q_lat[c, sl] for c in range(rank // LANES)], axis=1).astype(BF16)
        score[g] = (lax.dot_general(q_g, lat_g, across, preferred_element_type=F32)
                    + lax.dot_general(q_rope[0, sl, :rope_dim].astype(BF16), rope_g, across, preferred_element_type=F32))
    for g in range(groups):
        last = jnp.full((rows, keys), pos_ref[g * GROUP], jnp.int32)
        for i in range(1, GROUP):
            last = jnp.where(key_tok == i, pos_ref[g * GROUP + i], last)
        masked = jnp.where(same & (key_seq <= last), score[g] * head ** -0.5, -jnp.inf)
        expd = jnp.exp(masked - jnp.max(masked, axis=1, keepdims=True))
        prob[g] = (expd / jnp.sum(expd, axis=1, keepdims=True)).astype(BF16)
    for g in range(groups):
        sl, lat_g, _ = grouped(g)
        o_g = dot32(prob[g], lat_g).astype(BF16).astype(F32)
        for c in range(rank // LANES):
            o_lat[c, sl] = o_g[:, c * LANES:(c + 1) * LANES]
    lat_back.start()
    rope_back.start()

    uv_copy.wait()
    for n in range(n_heads):
        o_n = jnp.concatenate([o_lat[c, pl.ds(n, tok, stride=n_heads), :] for c in range(rank // LANES)], axis=1).astype(BF16)
        o_heads[:, n * uv.shape[2]:(n + 1) * uv.shape[2]] = dot32(o_n, uv[n]).astype(BF16)
    for i, copy in enumerate(wo_copies):
        copy.wait()
        for start, width in wide_tiles(dim // 2, 512):
            cols = slice(i * dim // 2 + start, i * dim // 2 + start + width)
            res_ref[:, cols] = (x[:, cols] + dot32(o_heads[...], wo[i, :, start:start + width])).astype(BF16)
    wr_copy.wait()
    h = (unit_norm(res_ref[...].astype(F32)) * fg_ref[...].astype(F32).reshape(1, dim)).astype(BF16)
    h_ref[...] = h

    gate = jax.nn.sigmoid(lax.dot_general(h, wr[...], across, preferred_element_type=F32))
    exp_row = lax.broadcasted_iota(jnp.int32, (n_exp, tok), 0)
    listed_t = jnp.zeros((n_exp, tok), F32)
    for i in range(ids_ref.shape[0]):
        listed_t = listed_t + jnp.where(exp_row == ids_ref[i:i + 1, :], 1.0, 0.0)
    listed_t = listed_t.astype(BF16)
    row, col = lax.broadcasted_iota(jnp.int32, (tok, tok), 0), lax.broadcasted_iota(jnp.int32, (tok, tok), 1)
    listed = lax.dot_general(jnp.where(row == col, 1.0, 0.0).astype(BF16), listed_t, across, preferred_element_type=F32)
    slots = lax.dot_general(jnp.where(row >= col, 1.0, 0.0).astype(BF16), listed_t, across, preferred_element_type=F32) * listed
    chosen = gate * listed
    table_ref[:, :n_exp] = ROUTE_SCALE * chosen / jnp.sum(chosen, axis=1, keepdims=True)
    table_ref[:, n_exp:] = slots
    lat_back.wait()
    rope_back.wait()


def attn_call(tok_in, lat_cache, rope_cache, tok_pos, expert_ids, attn_gain, w_query, w_kvdown, w_ukey, w_uval, w_out, ffn_gain, w_router):
    tok, dim = tok_in.shape
    n_heads, nope, rank = w_ukey.shape
    seq, rope_dim = rope_cache.shape[1:]
    n_exp = w_router.shape[1]
    blocks = n_heads // GROUP
    inv_freq = ROPE_BASE ** (-(2.0 * np.arange(rope_dim // 2)) / rope_dim)
    freq = jnp.asarray(inv_freq[None, :].astype(np.float32))
    vmem = pl.BlockSpec(memory_space=pltpu.VMEM)
    hbm = pl.BlockSpec(memory_space=pl.ANY)
    dma = pltpu.SemaphoreType.DMA
    return pl.pallas_call(
        attn_kernel,
        out_shape=[
            jax.ShapeDtypeStruct((tok, dim), BF16),
            jax.ShapeDtypeStruct((tok, dim), BF16),
            jax.ShapeDtypeStruct((tok, 2 * n_exp), F32),
            jax.ShapeDtypeStruct(lat_cache.shape, BF16),
            jax.ShapeDtypeStruct(rope_cache.shape, BF16),
        ],
        in_specs=[pl.BlockSpec(memory_space=pltpu.SMEM)] + [vmem] * 5 + [hbm] * 8,
        out_specs=[vmem, vmem, vmem, hbm, hbm],
        scratch_shapes=[
            pltpu.VMEM((blocks, dim, w_query.shape[1] // blocks), BF16),
            pltpu.VMEM(w_kvdown.shape[::-1], BF16),
            pltpu.VMEM(w_ukey.shape, BF16),
            pltpu.VMEM(w_uval.shape, BF16),
            pltpu.VMEM((2, w_out.shape[0], dim // 2), BF16),
            pltpu.VMEM(w_router.shape[::-1], BF16),
            pltpu.VMEM(lat_cache.shape, BF16),
            pltpu.VMEM(rope_cache.shape, BF16),
            pltpu.VMEM((rank // LANES, tok * n_heads, LANES), F32),
            pltpu.VMEM((1, tok * n_heads, LANES), F32),
            pltpu.VMEM((rank // LANES, tok * n_heads, LANES), F32),
            pltpu.VMEM((tok, w_out.shape[0]), BF16),
            pltpu.VMEM((tok // GROUP, GROUP * n_heads, GROUP * seq), F32),
            pltpu.VMEM((tok // GROUP, GROUP * n_heads, GROUP * seq), BF16),
            dma((blocks,)), dma((6,)), dma((2,)), dma((2,)),
        ],
        compiler_params=pltpu.CompilerParams(vmem_limit_bytes=60000000),
        name='latent_attention',
    )(tok_pos, tok_in, freq, expert_ids.T, attn_gain, ffn_gain, w_query, w_kvdown.T, w_ukey, w_uval, w_out, w_router.T, lat_cache, rope_cache)


def moe_kernel(n_ep, n_exp, h_ref, table_ref, resid_ref, rowpat_ref, colpat_ref,
               sg_ref, su_ref, sd_ref, eg_ref, eu_ref, ed_ref, out_ref,
               hall, gall, xg, act, act_sh, ebuf, esib, cmat, ct, ring, wa, wb, sh_out,
               sem_a, sem_b, ag_send, ag_recv, sib_send, sib_recv, tb_send, tb_recv, ts_send, ts_recv,
               ex_send, ex_recv, rg_send, rg_recv):
    nz = n_ep // 2
    far = nz // 2
    tok, dim = h_ref.shape
    e_loc, _, ff = eg_ref.shape
    halves = sg_ref.shape[1] // ff
    rows_par = nz * CAP
    rows_exp = 2 * rows_par
    rows_all = e_loc * rows_exp
    rows_q = e_loc * rows_par
    cw = dim // CHUNKS
    rw = dim // RINGS
    subs = RINGS // CHUNKS
    part_dim = dim // PARTS

    me = lax.axis_index('ep')
    z = me // 2
    par = lax.rem(me, 2)
    sib = me + 1 - 2 * par
    up_dev = lax.rem(z + 1, nz) * 2 + par
    dn_dev = lax.rem(z + nz - 1, nz) * 2 + par

    def chip(step):
        return lax.rem(z + step + 2 * nz, nz)

    def slot_of(p, zz):
        return p * nz + zz

    def a_slot(unit):
        return unit % SLOTS_A if unit < 2 * e_loc else unit - 2 * e_loc

    def a_copy(unit):
        slot = a_slot(unit)
        if unit < 2 * e_loc:
            src = (eg_ref if unit % 2 == 0 else eu_ref).at[unit // 2]
        else:
            hf = (unit - 2 * e_loc) // 2
            src = (sg_ref if unit % 2 == 0 else su_ref).at[:, pl.ds(hf * ff, ff)]
        return pltpu.make_async_copy(src, wa.at[slot], sem_a.at[unit])

    def b_place(unit):
        if unit >= CHUNKS * e_loc + SLOTS_B:
            pos = unit - CHUNKS * e_loc - SLOTS_B
            slot, side = 5 + pos // 2, pos % 2
        elif unit >= CHUNKS * e_loc:
            return wb.at[unit - CHUNKS * e_loc]
        elif unit >= SLOTS_B:
            slot, side = 1 + (unit - SLOTS_B) // 2, unit % 2
        else:
            return wb.at[unit]
        return wa.at[slot, pl.ds(0, ff), pl.ds(side * cw, cw)]

    def b_copy(unit):
        if unit < CHUNKS * e_loc:
            j, e = unit // e_loc, unit % e_loc
            src = ed_ref.at[e, :, pl.ds(j * cw, cw)]
        else:
            j, hf = (unit - CHUNKS * e_loc) // halves, (unit - CHUNKS * e_loc) % halves
            src = sd_ref.at[pl.ds(hf * ff, ff), pl.ds(j * cw, cw)]
        return pltpu.make_async_copy(src, b_place(unit), sem_b.at[unit])

    for unit in range(SLOTS_A):
        a_copy(unit).start()
    for unit in range(SLOTS_B):
        b_copy(unit).start()

    barrier = pltpu.get_barrier_semaphore()
    for dev in (up_dev, dn_dev, sib):
        pl.semaphore_signal(barrier, inc=1, device_id={'ep': dev}, device_id_type=MESH)
    pl.semaphore_wait(barrier, 3)

    def remote(src, dst, send, recv, dev):
        return pltpu.make_async_remote_copy(src_ref=src, dst_ref=dst, send_sem=send, recv_sem=recv,
                                            device_id={'ep': dev}, device_id_type=MESH)

    def h_hop(way, step, part):
        dev = up_dev if way == 0 else dn_dev
        origin = chip(-step if way == 0 else step)
        slot = slot_of(par, origin)
        cols = pl.ds(part * part_dim, part_dim)
        src = h_ref.at[:, cols] if step == 0 else hall.at[slot, :, cols]
        return remote(src, hall.at[slot, :, cols], ag_send.at[way, step, part], ag_recv.at[way, step, part], dev)

    def t_hop(way, step):
        dev = up_dev if way == 0 else dn_dev
        origin = chip(-step if way == 0 else step)
        slot = slot_of(par, origin)
        src = table_ref if step == 0 else gall.at[slot]
        return remote(src, gall.at[slot], tb_send.at[way, step], tb_recv.at[way, step], dev)

    def h_cross(k, origin):
        slot = slot_of(par, origin)
        src = h_ref if k == 0 else hall.at[slot]
        return remote(src, hall.at[slot], sib_send.at[k], sib_recv.at[k], sib)

    def t_cross(k, origin):
        slot = slot_of(par, origin)
        src = table_ref if k == 0 else gall.at[slot]
        return remote(src, gall.at[slot], ts_send.at[k], ts_recv.at[k], sib)

    t_steps = (far, far - 1)

    def place_rows():
        rowpat = rowpat_ref[...]
        row_exp, row_dev, row_slot = rowpat[:, 0:1], rowpat[:, 1:2], rowpat[:, 2:3]
        base = n_exp + e_loc * me
        lane = lax.broadcasted_iota(jnp.int32, (rows_all, LANES), 1)
        pick = jnp.where(lane == base + row_exp.astype(jnp.int32), 1.0, 0.0).astype(BF16)
        slots_by_row = lax.dot_general(pick, gall[...].reshape(n_ep * tok, LANES).astype(BF16), (((1,), (1,)), ((), ())),
                                       preferred_element_type=F32)
        tok_dev = (lax.broadcasted_iota(jnp.int32, (rows_all, n_ep * tok), 1) // tok).astype(F32)
        return jnp.where((slots_by_row == row_slot) & (tok_dev == row_dev), 1.0, 0.0).astype(BF16)

    def combine_weights():
        colpat = colpat_ref[...]
        col_exp, col_chip, col_slot = colpat[0:1, :], colpat[1:2, :], colpat[2:3, :]
        g_own = gall[pl.ds(par * nz, nz)].reshape(nz * tok, LANES)
        part1 = g_own.astype(BF16)
        rest1 = g_own - part1.astype(F32)
        part2 = rest1.astype(BF16)
        part3 = (rest1 - part2.astype(F32)).astype(BF16)
        sub = lax.broadcasted_iota(jnp.int32, (LANES, rows_q), 0)
        tok_chip = (lax.broadcasted_iota(jnp.int32, (nz * tok, rows_q), 0) // tok).astype(F32)
        for q in range(2):
            ids = e_loc * (me if q == 0 else sib) + col_exp.astype(jnp.int32)
            sel_w = jnp.where(sub == ids, 1.0, 0.0).astype(BF16)
            sel_s = jnp.where(sub == n_exp + ids, 1.0, 0.0).astype(BF16)
            here = (dot32(part1, sel_s) == col_slot) & (tok_chip == col_chip)
            for i, part in enumerate((part1, part2, part3)):
                cmat[q, i] = jnp.where(here, dot32(part, sel_w), 0.0).astype(BF16)
    sent = []

    def go(copy):
        copy.start()
        sent.append(copy)
        return copy

    hops, thops = {}, {}

    def goes(way, step, part):
        return step < far - 1 or part // (PARTS // 2) == way

    for way in range(2):
        thops[way, 0] = go(t_hop(way, 0))
    for part in range(PARTS):
        for way in range(2):
            hops[way, 0, part] = go(h_hop(way, 0, part))
    t_crossed, h_crossed = [go(t_cross(0, z))], [go(h_cross(0, z))]
    hall[slot_of(par, z)] = h_ref[...]
    gall[slot_of(par, z)] = table_ref[...]
    for step in range(far):
        for way in range(2):
            if step < t_steps[way]:
                origin = chip(-(step + 1) if way == 0 else step + 1)
                thops[way, step].wait_recv()
                if step + 1 < t_steps[way]:
                    thops[way, step + 1] = go(t_hop(way, step + 1))
                t_crossed.append(go(t_cross(1 + 2 * step + way, origin)))
        if step == far - 1:
            for copy in t_crossed:
                copy.wait_recv()
            place = place_rows()
            combine_weights()
        for part in range(PARTS):
            for way in range(2):
                if goes(way, step, part):
                    hops[way, step, part].wait_recv()
                    if step + 1 < far and goes(way, step + 1, part):
                        hops[way, step + 1, part] = go(h_hop(way, step + 1, part))
        if step < far - 1:
            for way in range(2):
                h_crossed.append(go(h_cross(1 + 2 * step + way, chip(-(step + 1) if way == 0 else step + 1))))
    h_crossed.append(go(h_cross(2 * far - 1, chip(far))))
    for copy in h_crossed:
        copy.wait_recv()
    for start, width in wide_tiles(dim, 256):
        rows = hall[:, :, start:start + width].reshape(n_ep * tok, width)
        xg[:, :, start:start + width] = dot32(place, rows).astype(BF16).reshape(e_loc, rows_exp, width)

    def swiglu_tile(x, slot_g, slot_u, start, width):
        gate = dot32(x, wa[slot_g, :, start:start + width])
        up = dot32(x, wa[slot_u, :, start:start + width])
        return (jax.nn.silu(gate) * up).astype(BF16)

    def expert_up(e, carry):
        slot_g = lax.rem(2 * e, SLOTS_A)
        slot_u = lax.rem(2 * e + 1, SLOTS_A)
        for unit, slot in ((2 * e, slot_g), (2 * e + 1, slot_u)):
            pltpu.make_async_copy(eg_ref.at[0], wa.at[slot], sem_a.at[unit]).wait()
        for start, width in wide_tiles(ff, TILE):
            act[e, :, start:start + width] = swiglu_tile(xg[e], slot_g, slot_u, start, width)
        for e_st in range(e_loc):
            @pl.when(e == e_st)
            def _():
                if e_st == 0:
                    a_copy(SLOTS_A).start()
                    ahead = (4, 5)
                elif e_st < e_loc - 1:
                    ahead = range(4 * e_st + 2, 4 * e_st + 6)
                else:
                    ahead = (14, 15)
                for unit in ahead:
                    b_copy(unit).start()
                if e_st == e_loc - 1:
                    a_copy(2 * e_loc).start()
        return carry

    lax.fori_loop(0, e_loc, expert_up, 0)

    def reach(way, j):
        return far if (way + j) % 2 == 0 else nz - 1 - far

    def ring_copy(way, j, step):
        dev = up_dev if way == 0 else dn_dev
        ahead = reach(way, j) - step + 1
        dest = chip(ahead if way == 0 else -ahead)
        src = ct.at[j, dest] if step == 1 else ring.at[way, j, step - 2]
        return remote(src, ring.at[way, j, step - 1], rg_send.at[way, j, step - 1], rg_recv.at[way, j, step - 1], dev)

    rcopies = {}

    def combine(j):
        exch[j].wait_recv()
        own = ebuf[j, par].reshape(rows_q, rw)
        other = esib[j].reshape(rows_q, rw)
        total = dot32(cmat[0, 0], own) + dot32(cmat[1, 0], other)
        for i in (1, 2):
            total += dot32(cmat[0, i], own) + dot32(cmat[1, i], other)
        ct[j] = total.reshape(nz, tok, rw)
        for way in range(2):
            rcopies[way, j, 1] = go(ring_copy(way, j, 1))

    def advance(j, step):
        for way in range(2):
            if step < reach(way, j):
                rcopies[way, j, step].wait_recv()
                ahead = reach(way, j) - step
                dest = chip(ahead if way == 0 else -ahead)
                ring[way, j, step - 1] += ct[j, dest]
                rcopies[way, j, step + 1] = go(ring_copy(way, j, step + 1))

    def finish(j):
        cols = slice(j * rw, (j + 1) * rw)
        total = resid_ref[:, cols].astype(F32) + sh_out[:, cols] + ct[j, z]
        for way in range(2):
            rcopies[way, j, reach(way, j)].wait_recv()
            total += ring[way, j, reach(way, j) - 1]
        out_ref[:, cols] = total

    exch = {}

    def down(r):
        j, sub = r // subs, r % subs
        if sub == 0:
            for e in range(e_loc):
                b_copy(j * e_loc + e).wait()
        for e in range(e_loc):
            res = dot32(act[e], b_place(j * e_loc + e)[:, sub * rw:(sub + 1) * rw]).astype(BF16)
            ebuf[r, 0, e] = res[:rows_par]
            ebuf[r, 1, e] = res[rows_par:]
        exch[r] = go(remote(ebuf.at[r, 1 - par], esib.at[r], ex_send.at[r], ex_recv.at[r], sib))
        if sub < subs - 1:
            return
        shared = CHUNKS * e_loc
        if j == 1:
            a_copy(2 * e_loc + 1).start()
            a_copy(2 * e_loc + 2).start()
        elif j == 2:
            a_copy(2 * e_loc + 3).start()
            for pos in range(SLOTS_B):
                b_copy(shared + pos).start()
        elif j == 3:
            for pos in range(SLOTS_B, CHUNKS * halves):
                b_copy(shared + pos).start()

    def shared_up(hf, tile):
        unit = 2 * e_loc + 2 * hf
        start, width = wide_tiles(ff, TILE)[tile]
        if tile == 0:
            a_copy(unit).wait()
            a_copy(unit + 1).wait()
        act_sh[hf, :, start:start + width] = swiglu_tile(h_ref[...], a_slot(unit), a_slot(unit + 1), start, width)

    def shared_down(j):
        total = jnp.zeros((tok, cw), F32)
        for hf in range(halves):
            unit = CHUNKS * e_loc + j * halves + hf
            b_copy(unit).wait()
            total += dot32(act_sh[hf], b_place(unit)[...])
        sh_out[:, j * cw:(j + 1) * cw] = total

    down(0)
    down(1)
    for r in range(2, RINGS):
        down(r)
        combine(r - 2)
    combine(RINGS - 2)
    combine(RINGS - 1)
    tiles = len(wide_tiles(ff, TILE))
    pieces = [functools.partial(shared_up, hf, tile) for hf in range(halves) for tile in range(tiles)]
    pieces += [functools.partial(shared_down, j) for j in range(CHUNKS)]
    events = [(j, step) for step in range(1, far) for j in range(RINGS)]
    for i, event in enumerate(events):
        advance(*event)
        for piece in pieces[i * len(pieces) // len(events):(i + 1) * len(pieces) // len(events)]:
            piece()
    for j in range(RINGS):
        finish(j)
    for copy in sent:
        copy.wait_send()


def moe_call(n_ep, h_norm, table, resid, w_sg, w_su, w_sd, w_eg, w_eu, w_ed):
    nz = n_ep // 2
    tok, dim = h_norm.shape
    e_loc, _, ff = w_eg.shape
    n_exp = e_loc * n_ep
    halves = w_sg.shape[1] // ff
    far = nz // 2
    cw = dim // CHUNKS
    rw = dim // RINGS
    rows_par = nz * CAP
    rows_exp = 2 * rows_par
    rows_all = e_loc * rows_exp
    rows_q = e_loc * rows_par
    row = np.arange(rows_all)
    rowpat = np.zeros((rows_all, 8), np.float32)
    rowpat[:, 0] = row // rows_exp
    rowpat[:, 1] = (row % rows_exp) // CAP
    rowpat[:, 2] = row % CAP + 1
    col = np.arange(rows_q)
    colpat = np.zeros((8, rows_q), np.float32)
    colpat[0] = col // rows_par
    colpat[1] = (col % rows_par) // CAP
    colpat[2] = col % CAP + 1
    vmem = pl.BlockSpec(memory_space=pltpu.VMEM)
    hbm = pl.BlockSpec(memory_space=pl.ANY)
    dma = pltpu.SemaphoreType.DMA
    return pl.pallas_call(
        functools.partial(moe_kernel, n_ep, n_exp),
        out_shape=jax.ShapeDtypeStruct((tok, dim), F32),
        in_specs=[vmem] * 5 + [hbm] * 6,
        out_specs=vmem,
        scratch_shapes=[
            pltpu.VMEM((n_ep, tok, dim), BF16),
            pltpu.VMEM((n_ep, tok, LANES), F32),
            pltpu.VMEM((e_loc, rows_exp, dim), BF16),
            pltpu.VMEM((e_loc, rows_exp, ff), BF16),
            pltpu.VMEM((halves, tok, ff), BF16),
            pltpu.VMEM((RINGS, 2, e_loc, rows_par, rw), BF16),
            pltpu.VMEM((RINGS, e_loc, rows_par, rw), BF16),
            pltpu.VMEM((2, 3, nz * tok, rows_q), BF16),
            pltpu.VMEM((RINGS, nz, tok, rw), F32),
            pltpu.VMEM((2, RINGS, far, tok, rw), F32),
            pltpu.VMEM((SLOTS_A, dim, ff), BF16),
            pltpu.VMEM((SLOTS_B, ff, cw), BF16),
            pltpu.VMEM((tok, dim), F32),
            dma((2 * (e_loc + halves),)), dma((CHUNKS * (e_loc + halves),)),
            dma((2, far, PARTS)), dma((2, far, PARTS)), dma((nz,)), dma((nz,)),
            dma((2, far)), dma((2, far)), dma((nz,)), dma((nz,)),
            dma((RINGS,)), dma((RINGS,)),
            dma((2, RINGS, far)), dma((2, RINGS, far)),
        ],
        compiler_params=pltpu.CompilerParams(collective_id=0, has_side_effects=True, vmem_limit_bytes=67000000),
        name='moe_ring',
    )(h_norm, table, resid, jnp.asarray(rowpat), jnp.asarray(colpat), w_sg, w_su, w_sd, w_eg, w_eu, w_ed).astype(BF16)


def solution(mesh):
    n_ep = mesh.shape['ep']
    row_one = P(('dp', 'ep'))
    row_two = P(('dp', 'ep'), None)
    row_three = P(('dp', 'ep'), None, None)
    rep_one = P(None)
    rep_two = P(None, None)
    rep_three = P(None, None, None)
    exp_spec = P('ep', None, None)

    def local_step(tok_in, lat_cache, rope_cache, tok_pos, expert_ids, attn_gain, w_query, w_kvdown, w_ukey, w_uval, w_out, ffn_gain, w_router, sh_gate, sh_up, sh_down, ex_gate, ex_up, ex_down):
        resid_bf, h_norm, table, lat_out, rope_out = attn_call(tok_in, lat_cache, rope_cache, tok_pos, expert_ids, attn_gain, w_query, w_kvdown, w_ukey, w_uval, w_out, ffn_gain, w_router)
        out_hidden = moe_call(n_ep, h_norm, table, resid_bf, sh_gate, sh_up, sh_down, ex_gate, ex_up, ex_down)
        return out_hidden, lat_out, rope_out

    in_specs = (row_two, row_three, row_three, row_one, row_two, rep_one, rep_two, rep_two, rep_three, rep_three, rep_two, rep_one, rep_two, rep_two, rep_two, rep_two, exp_spec, exp_spec, exp_spec)
    out_specs = (row_two, row_three, row_three)
    return jax.shard_map(local_step, mesh=mesh, in_specs=in_specs, out_specs=out_specs, check_vma=False)
```

```python
import functools

import jax
import jax.numpy as jnp
import numpy as np
from jax import lax
from jax.experimental import pallas as pl
from jax.experimental.pallas import tpu as pltpu
from jax.sharding import PartitionSpec as P

ROUTE_SCALE = 2.827
ROPE_BASE = 10000.0
NORM_EPS = 1e-6
MESH = pl.DeviceIdType.MESH
F32 = jnp.float32
BF16 = jnp.bfloat16
CHUNKS = 4
RINGS = 4
TILE = 256
SLOTS_A = 7
SLOTS_B = 4
CAP = 6
PARTS = 4
LANES = 128
GROUP = 4


def unit_norm(values):
    mean_sq = jnp.mean(jnp.square(values), axis=-1, keepdims=True)
    return values * lax.rsqrt(mean_sq + NORM_EPS)


def dot32(lhs, rhs):
    return jnp.dot(lhs, rhs, preferred_element_type=F32)


def wide_tiles(total, width):
    return [(start, min(width, total - start)) for start in range(0, total, width)]


def attn_kernel(pos_hbm, x_hbm, freq_hbm, ids_hbm, ag_hbm, fg_hbm, wq_ref, wkv_ref, uk_ref, uv_ref, wo_ref, wr_ref, lat_ref, rope_ref,
                res_ref, h_ref, table_ref, lat_out, rope_out,
                wq, wkv, uk, uv, wo, wr, lat, rope, q_lat, q_rope, o_lat, o_heads, score, prob, pos_ref, x_ref, freq_ref, ids_ref, ag_ref, fg_ref, sem_q, sem_w, sem_c, sem_o, sem_i):
    n_heads, nope, rank = uk_ref.shape
    tok, dim = x_ref.shape
    seq, rope_dim = rope_ref.shape[1:]
    half = rope_dim // 2
    head = nope + rope_dim
    n_exp = wr_ref.shape[0]
    blocks = n_heads // GROUP
    q_cols = GROUP * head

    def q_copy(blk):
        return pltpu.make_async_copy(wq_ref.at[:, pl.ds(blk * q_cols, q_cols)], wq.at[blk], sem_q.at[blk])

    kv_copy = pltpu.make_async_copy(wkv_ref, wkv, sem_w.at[0])
    uk_copy = pltpu.make_async_copy(uk_ref, uk, sem_w.at[1])
    uv_copy = pltpu.make_async_copy(uv_ref, uv, sem_w.at[2])
    wo_copies = [pltpu.make_async_copy(wo_ref.at[:, pl.ds(i * dim // 2, dim // 2)], wo.at[i], sem_w.at[3 + i]) for i in range(2)]
    wr_copy = pltpu.make_async_copy(wr_ref, wr, sem_w.at[5])
    lat_copy = pltpu.make_async_copy(lat_ref, lat, sem_c.at[0])
    rope_copy = pltpu.make_async_copy(rope_ref, rope, sem_c.at[1])
    small = [pltpu.make_async_copy(src, dst, sem_i.at[i]) for i, (src, dst) in enumerate((
        (x_hbm, x_ref), (ag_hbm, ag_ref), (pos_hbm, pos_ref), (freq_hbm, freq_ref), (fg_hbm, fg_ref), (ids_hbm, ids_ref)))]
    for copy in small[:4]:
        copy.start()
    kv_copy.start()
    q_copy(0).start()
    uk_copy.start()
    q_copy(1).start()
    for copy in small[4:]:
        copy.start()
    for copy in small:
        copy.wait()

    x = x_ref[...].astype(F32)
    x_norm = (unit_norm(x) * ag_ref[...].astype(F32).reshape(1, dim)).astype(BF16)
    tok_row = lax.broadcasted_iota(jnp.int32, (tok, half), 0)
    pos = jnp.zeros((tok, half), jnp.int32)
    for t in range(tok):
        pos = jnp.where(tok_row == t, pos_ref[t], pos)
    angle = pos.astype(F32) * freq_ref[...]
    cos, sin = jnp.cos(angle), jnp.sin(angle)
    across = (((1,), (1,)), ((), ()))

    def rotate(first, second):
        return jnp.concatenate([first * cos - second * sin, second * cos + first * sin], axis=1)

    kv_copy.wait()
    for blk in range(2, blocks):
        q_copy(blk).start()
    kv = lax.dot_general(x_norm, wkv[...], across, preferred_element_type=F32)
    lat_new = unit_norm(kv[:, :rank]).astype(BF16).astype(F32)
    rope_new = rotate(kv[:, rank:rank + half], kv[:, rank + half:]).astype(BF16).astype(F32)

    def spread(ref, n, val):
        for c in range(val.shape[1] // LANES):
            ref[c, pl.ds(n, tok, stride=n_heads), :] = val[:, c * LANES:(c + 1) * LANES]

    queries = []

    def heads(blk):
        q = queries[blk]
        for i in range(GROUP):
            n = blk * GROUP + i
            at = i * head
            spread(q_lat, n, dot32(q[:, at:at + nope], uk[n]).astype(BF16).astype(F32))
            q_r = q[:, at + nope:at + head].astype(F32)
            q_r = rotate(q_r[:, :half], q_r[:, half:]).astype(BF16).astype(F32)
            spread(q_rope, n, jnp.concatenate([q_r, jnp.zeros((tok, LANES - rope_dim), F32)], axis=1))

    uk_copy.wait()
    for blk in range(blocks):
        q_copy(blk).wait()
        if blk == 0:
            lat_copy.start()
            rope_copy.start()
            uv_copy.start()
        elif blk == 1:
            wr_copy.start()
            for copy in wo_copies:
                copy.start()
        queries.append(dot32(x_norm, wq[blk]).astype(BF16))
        if blk > 0:
            heads(blk - 1)
    lat_copy.wait()
    rope_copy.wait()
    heads(blocks - 1)
    rows, keys = GROUP * n_heads, GROUP * seq
    key = lax.broadcasted_iota(jnp.int32, (rows, keys), 1)
    same = (key // seq) == (lax.broadcasted_iota(jnp.int32, (rows, keys), 0) // n_heads)
    key_tok, key_seq = key // seq, lax.rem(key, seq)
    groups = tok // GROUP

    def grouped(g):
        lat_g = lat[g * GROUP:(g + 1) * GROUP].reshape(keys, rank)
        rope_g = rope[g * GROUP:(g + 1) * GROUP].reshape(keys, rope_dim)
        return slice(g * rows, (g + 1) * rows), lat_g, rope_g

    lat_row = lax.broadcasted_iota(jnp.int32, (seq, rank), 0)
    rope_row = lax.broadcasted_iota(jnp.int32, (seq, rope_dim), 0)
    for t in range(tok):
        lat[t] = jnp.where(lat_row == pos_ref[t], lat_new[t:t + 1], lat[t].astype(F32)).astype(BF16)
        rope[t] = jnp.where(rope_row == pos_ref[t], rope_new[t:t + 1], rope[t].astype(F32)).astype(BF16)
    lat_back = pltpu.make_async_copy(lat, lat_out, sem_o.at[0])
    rope_back = pltpu.make_async_copy(rope, rope_out, sem_o.at[1])
    for g in range(groups):
        sl, lat_g, rope_g = grouped(g)
        q_g = jnp.concatenate([q_lat[c, sl] for c in range(rank // LANES)], axis=1).astype(BF16)
        score[g] = (lax.dot_general(q_g, lat_g, across, preferred_element_type=F32)
                    + lax.dot_general(q_rope[0, sl, :rope_dim].astype(BF16), rope_g, across, preferred_element_type=F32))
    for g in range(groups):
        last = jnp.full((rows, keys), pos_ref[g * GROUP], jnp.int32)
        for i in range(1, GROUP):
            last = jnp.where(key_tok == i, pos_ref[g * GROUP + i], last)
        masked = jnp.where(same & (key_seq <= last), score[g] * head ** -0.5, -jnp.inf)
        expd = jnp.exp(masked - jnp.max(masked, axis=1, keepdims=True))
        prob[g] = (expd / jnp.sum(expd, axis=1, keepdims=True)).astype(BF16)
    for g in range(groups):
        sl, lat_g, _ = grouped(g)
        o_g = dot32(prob[g], lat_g).astype(BF16).astype(F32)
        for c in range(rank // LANES):
            o_lat[c, sl] = o_g[:, c * LANES:(c + 1) * LANES]
    lat_back.start()
    rope_back.start()

    uv_copy.wait()
    for n in range(n_heads):
        o_n = jnp.concatenate([o_lat[c, pl.ds(n, tok, stride=n_heads), :] for c in range(rank // LANES)], axis=1).astype(BF16)
        o_heads[:, n * uv.shape[2]:(n + 1) * uv.shape[2]] = dot32(o_n, uv[n]).astype(BF16)
    for i, copy in enumerate(wo_copies):
        copy.wait()
        for start, width in wide_tiles(dim // 2, 512):
            cols = slice(i * dim // 2 + start, i * dim // 2 + start + width)
            res_ref[:, cols] = (x[:, cols] + dot32(o_heads[...], wo[i, :, start:start + width])).astype(BF16)
    wr_copy.wait()
    h = (unit_norm(res_ref[...].astype(F32)) * fg_ref[...].astype(F32).reshape(1, dim)).astype(BF16)
    h_ref[...] = h

    gate = jax.nn.sigmoid(lax.dot_general(h, wr[...], across, preferred_element_type=F32))
    exp_row = lax.broadcasted_iota(jnp.int32, (n_exp, tok), 0)
    listed_t = jnp.zeros((n_exp, tok), F32)
    for i in range(ids_ref.shape[0]):
        listed_t = listed_t + jnp.where(exp_row == ids_ref[i:i + 1, :], 1.0, 0.0)
    listed_t = listed_t.astype(BF16)
    row, col = lax.broadcasted_iota(jnp.int32, (tok, tok), 0), lax.broadcasted_iota(jnp.int32, (tok, tok), 1)
    listed = lax.dot_general(jnp.where(row == col, 1.0, 0.0).astype(BF16), listed_t, across, preferred_element_type=F32)
    slots = lax.dot_general(jnp.where(row >= col, 1.0, 0.0).astype(BF16), listed_t, across, preferred_element_type=F32) * listed
    chosen = gate * listed
    table_ref[:, :n_exp] = ROUTE_SCALE * chosen / jnp.sum(chosen, axis=1, keepdims=True)
    table_ref[:, n_exp:] = slots
    lat_back.wait()
    rope_back.wait()


def attn_call(tok_in, lat_cache, rope_cache, tok_pos, expert_ids, attn_gain, w_query, w_kvdown, w_ukey, w_uval, w_out, ffn_gain, w_router):
    tok, dim = tok_in.shape
    n_heads, nope, rank = w_ukey.shape
    seq, rope_dim = rope_cache.shape[1:]
    n_exp = w_router.shape[1]
    blocks = n_heads // GROUP
    inv_freq = ROPE_BASE ** (-(2.0 * np.arange(rope_dim // 2)) / rope_dim)
    freq = jnp.asarray(inv_freq[None, :].astype(np.float32))
    vmem = pl.BlockSpec(memory_space=pltpu.VMEM)
    hbm = pl.BlockSpec(memory_space=pl.ANY)
    dma = pltpu.SemaphoreType.DMA
    return pl.pallas_call(
        attn_kernel,
        out_shape=[
            jax.ShapeDtypeStruct((tok, dim), BF16),
            jax.ShapeDtypeStruct((tok, dim), BF16),
            jax.ShapeDtypeStruct((tok, 2 * n_exp), F32),
            jax.ShapeDtypeStruct(lat_cache.shape, BF16),
            jax.ShapeDtypeStruct(rope_cache.shape, BF16),
        ],
        in_specs=[hbm] * 14,
        out_specs=[vmem, vmem, vmem, hbm, hbm],
        scratch_shapes=[
            pltpu.VMEM((blocks, dim, w_query.shape[1] // blocks), BF16),
            pltpu.VMEM(w_kvdown.shape[::-1], BF16),
            pltpu.VMEM(w_ukey.shape, BF16),
            pltpu.VMEM(w_uval.shape, BF16),
            pltpu.VMEM((2, w_out.shape[0], dim // 2), BF16),
            pltpu.VMEM(w_router.shape[::-1], BF16),
            pltpu.VMEM(lat_cache.shape, BF16),
            pltpu.VMEM(rope_cache.shape, BF16),
            pltpu.VMEM((rank // LANES, tok * n_heads, LANES), F32),
            pltpu.VMEM((1, tok * n_heads, LANES), F32),
            pltpu.VMEM((rank // LANES, tok * n_heads, LANES), F32),
            pltpu.VMEM((tok, w_out.shape[0]), BF16),
            pltpu.VMEM((tok // GROUP, GROUP * n_heads, GROUP * seq), F32),
            pltpu.VMEM((tok // GROUP, GROUP * n_heads, GROUP * seq), BF16),
            pltpu.SMEM(tok_pos.shape, jnp.int32),
            pltpu.VMEM((tok, dim), BF16),
            pltpu.VMEM(freq.shape, F32),
            pltpu.VMEM(expert_ids.shape[::-1], jnp.int32),
            pltpu.VMEM((dim,), BF16),
            pltpu.VMEM((dim,), BF16),
            dma((blocks,)), dma((6,)), dma((2,)), dma((2,)), dma((6,)),
        ],
        compiler_params=pltpu.CompilerParams(vmem_limit_bytes=60000000),
        name='latent_attention',
    )(tok_pos, tok_in, freq, expert_ids.T, attn_gain, ffn_gain, w_query, w_kvdown.T, w_ukey, w_uval, w_out, w_router.T, lat_cache, rope_cache)


def moe_kernel(n_ep, n_exp, h_hbm, table_hbm, resid_hbm, rowpat_hbm, colpat_hbm,
               sg_ref, su_ref, sd_ref, eg_ref, eu_ref, ed_ref, out_hbm,
               hall, gall, xg, act, act_sh, ebuf, esib, cmat, ct, ring, wa, wb, sh_out,
               sem_a, sem_b, ag_send, ag_recv, sib_send, sib_recv, tb_send, tb_recv, ts_send, ts_recv,
               ex_send, ex_recv, rg_send, rg_recv, h_ref, table_ref, resid_ref, rowpat_ref, colpat_ref, out_ref, sem_i, sem_o):
    nz = n_ep // 2
    far = nz // 2
    tok, dim = h_hbm.shape
    e_loc, _, ff = eg_ref.shape
    halves = sg_ref.shape[1] // ff
    rows_par = nz * CAP
    rows_exp = 2 * rows_par
    rows_all = e_loc * rows_exp
    rows_q = e_loc * rows_par
    cw = dim // CHUNKS
    rw = dim // RINGS
    subs = RINGS // CHUNKS
    part_dim = dim // PARTS

    me = lax.axis_index('ep')
    z = me // 2
    par = lax.rem(me, 2)
    sib = me + 1 - 2 * par
    up_dev = lax.rem(z + 1, nz) * 2 + par
    dn_dev = lax.rem(z + nz - 1, nz) * 2 + par

    def chip(step):
        return lax.rem(z + step + 2 * nz, nz)

    def slot_of(p, zz):
        return p * nz + zz

    def a_slot(unit):
        return unit % SLOTS_A if unit < 2 * e_loc else unit - 2 * e_loc

    def a_copy(unit):
        slot = a_slot(unit)
        if unit < 2 * e_loc:
            src = (eg_ref if unit % 2 == 0 else eu_ref).at[unit // 2]
        else:
            hf = (unit - 2 * e_loc) // 2
            src = (sg_ref if unit % 2 == 0 else su_ref).at[:, pl.ds(hf * ff, ff)]
        return pltpu.make_async_copy(src, wa.at[slot], sem_a.at[unit])

    def b_place(unit):
        if unit >= CHUNKS * e_loc + SLOTS_B:
            pos = unit - CHUNKS * e_loc - SLOTS_B
            slot, side = 5 + pos // 2, pos % 2
        elif unit >= CHUNKS * e_loc:
            return wb.at[unit - CHUNKS * e_loc]
        elif unit >= SLOTS_B:
            slot, side = 1 + (unit - SLOTS_B) // 2, unit % 2
        else:
            return wb.at[unit]
        return wa.at[slot, pl.ds(0, ff), pl.ds(side * cw, cw)]

    def b_copy(unit):
        if unit < CHUNKS * e_loc:
            j, e = unit // e_loc, unit % e_loc
            src = ed_ref.at[e, :, pl.ds(j * cw, cw)]
        else:
            j, hf = (unit - CHUNKS * e_loc) // halves, (unit - CHUNKS * e_loc) % halves
            src = sd_ref.at[pl.ds(hf * ff, ff), pl.ds(j * cw, cw)]
        return pltpu.make_async_copy(src, b_place(unit), sem_b.at[unit])

    small = [pltpu.make_async_copy(src, dst, sem_i.at[i]) for i, (src, dst) in enumerate((
        (table_hbm, table_ref), (h_hbm, h_ref), (resid_hbm, resid_ref), (rowpat_hbm, rowpat_ref), (colpat_hbm, colpat_ref)))]
    for copy in small:
        copy.start()

    barrier = pltpu.get_barrier_semaphore()
    for dev in (up_dev, dn_dev, sib):
        pl.semaphore_signal(barrier, inc=1, device_id={'ep': dev}, device_id_type=MESH)
    for unit in range(SLOTS_A):
        a_copy(unit).start()
    for unit in range(SLOTS_B):
        b_copy(unit).start()
    for copy in small:
        copy.wait()
    pl.semaphore_wait(barrier, 3)

    def remote(src, dst, send, recv, dev):
        return pltpu.make_async_remote_copy(src_ref=src, dst_ref=dst, send_sem=send, recv_sem=recv,
                                            device_id={'ep': dev}, device_id_type=MESH)

    def h_hop(way, step, part):
        dev = up_dev if way == 0 else dn_dev
        origin = chip(-step if way == 0 else step)
        slot = slot_of(par, origin)
        cols = pl.ds(part * part_dim, part_dim)
        src = h_ref.at[:, cols] if step == 0 else hall.at[slot, :, cols]
        return remote(src, hall.at[slot, :, cols], ag_send.at[way, step, part], ag_recv.at[way, step, part], dev)

    def t_hop(way, step):
        dev = up_dev if way == 0 else dn_dev
        origin = chip(-step if way == 0 else step)
        slot = slot_of(par, origin)
        src = table_ref if step == 0 else gall.at[slot]
        return remote(src, gall.at[slot], tb_send.at[way, step], tb_recv.at[way, step], dev)

    def h_cross(k, origin):
        slot = slot_of(par, origin)
        src = h_ref if k == 0 else hall.at[slot]
        return remote(src, hall.at[slot], sib_send.at[k], sib_recv.at[k], sib)

    def t_cross(k, origin):
        slot = slot_of(par, origin)
        src = table_ref if k == 0 else gall.at[slot]
        return remote(src, gall.at[slot], ts_send.at[k], ts_recv.at[k], sib)

    t_steps = (far, far - 1)

    def place_rows():
        rowpat = rowpat_ref[...]
        row_exp, row_dev, row_slot = rowpat[:, 0:1], rowpat[:, 1:2], rowpat[:, 2:3]
        base = n_exp + e_loc * me
        lane = lax.broadcasted_iota(jnp.int32, (rows_all, LANES), 1)
        pick = jnp.where(lane == base + row_exp.astype(jnp.int32), 1.0, 0.0).astype(BF16)
        slots_by_row = lax.dot_general(pick, gall[...].reshape(n_ep * tok, LANES).astype(BF16), (((1,), (1,)), ((), ())),
                                       preferred_element_type=F32)
        tok_dev = (lax.broadcasted_iota(jnp.int32, (rows_all, n_ep * tok), 1) // tok).astype(F32)
        return jnp.where((slots_by_row == row_slot) & (tok_dev == row_dev), 1.0, 0.0).astype(BF16)

    def combine_weights():
        colpat = colpat_ref[...]
        col_exp, col_chip, col_slot = colpat[0:1, :], colpat[1:2, :], colpat[2:3, :]
        g_own = gall[pl.ds(par * nz, nz)].reshape(nz * tok, LANES)
        part1 = g_own.astype(BF16)
        rest1 = g_own - part1.astype(F32)
        part2 = rest1.astype(BF16)
        part3 = (rest1 - part2.astype(F32)).astype(BF16)
        sub = lax.broadcasted_iota(jnp.int32, (LANES, rows_q), 0)
        tok_chip = (lax.broadcasted_iota(jnp.int32, (nz * tok, rows_q), 0) // tok).astype(F32)
        for q in range(2):
            ids = e_loc * (me if q == 0 else sib) + col_exp.astype(jnp.int32)
            sel_w = jnp.where(sub == ids, 1.0, 0.0).astype(BF16)
            sel_s = jnp.where(sub == n_exp + ids, 1.0, 0.0).astype(BF16)
            here = (dot32(part1, sel_s) == col_slot) & (tok_chip == col_chip)
            for i, part in enumerate((part1, part2, part3)):
                cmat[q, i] = jnp.where(here, dot32(part, sel_w), 0.0).astype(BF16)
    sent = []

    def go(copy):
        copy.start()
        sent.append(copy)
        return copy

    hops, thops = {}, {}

    def goes(way, step, part):
        return step < far - 1 or part // (PARTS // 2) == way

    for way in range(2):
        thops[way, 0] = go(t_hop(way, 0))
    for part in range(PARTS):
        for way in range(2):
            hops[way, 0, part] = go(h_hop(way, 0, part))
    t_crossed, h_crossed = [go(t_cross(0, z))], [go(h_cross(0, z))]
    hall[slot_of(par, z)] = h_ref[...]
    gall[slot_of(par, z)] = table_ref[...]
    for step in range(far):
        for way in range(2):
            if step < t_steps[way]:
                origin = chip(-(step + 1) if way == 0 else step + 1)
                thops[way, step].wait_recv()
                if step + 1 < t_steps[way]:
                    thops[way, step + 1] = go(t_hop(way, step + 1))
                t_crossed.append(go(t_cross(1 + 2 * step + way, origin)))
        if step == far - 1:
            for copy in t_crossed:
                copy.wait_recv()
            place = place_rows()
            combine_weights()
        for part in range(PARTS):
            for way in range(2):
                if goes(way, step, part):
                    hops[way, step, part].wait_recv()
                    if step + 1 < far and goes(way, step + 1, part):
                        hops[way, step + 1, part] = go(h_hop(way, step + 1, part))
        if step < far - 1:
            for way in range(2):
                h_crossed.append(go(h_cross(1 + 2 * step + way, chip(-(step + 1) if way == 0 else step + 1))))
    h_crossed.append(go(h_cross(2 * far - 1, chip(far))))
    for copy in h_crossed:
        copy.wait_recv()
    for start, width in wide_tiles(dim, 256):
        rows = hall[:, :, start:start + width].reshape(n_ep * tok, width)
        xg[:, :, start:start + width] = dot32(place, rows).astype(BF16).reshape(e_loc, rows_exp, width)

    def swiglu_tile(x, slot_g, slot_u, start, width):
        gate = dot32(x, wa[slot_g, :, start:start + width])
        up = dot32(x, wa[slot_u, :, start:start + width])
        return (jax.nn.silu(gate) * up).astype(BF16)

    def expert_up(e, carry):
        slot_g = lax.rem(2 * e, SLOTS_A)
        slot_u = lax.rem(2 * e + 1, SLOTS_A)
        for unit, slot in ((2 * e, slot_g), (2 * e + 1, slot_u)):
            pltpu.make_async_copy(eg_ref.at[0], wa.at[slot], sem_a.at[unit]).wait()
        for start, width in wide_tiles(ff, TILE):
            act[e, :, start:start + width] = swiglu_tile(xg[e], slot_g, slot_u, start, width)
        for e_st in range(e_loc):
            @pl.when(e == e_st)
            def _():
                if e_st == 0:
                    a_copy(SLOTS_A).start()
                    ahead = (4, 5)
                elif e_st < e_loc - 1:
                    ahead = range(4 * e_st + 2, 4 * e_st + 6)
                else:
                    ahead = (14, 15)
                for unit in ahead:
                    b_copy(unit).start()
                if e_st == e_loc - 1:
                    a_copy(2 * e_loc).start()
        return carry

    lax.fori_loop(0, e_loc, expert_up, 0)

    def reach(way, j):
        return far if (way + j) % 2 == 0 else nz - 1 - far

    def ring_copy(way, j, step):
        dev = up_dev if way == 0 else dn_dev
        ahead = reach(way, j) - step + 1
        dest = chip(ahead if way == 0 else -ahead)
        src = ct.at[j // subs, dest, :, pl.ds(j % subs * rw, rw)] if step == 1 else ring.at[way, j, step - 2]
        return remote(src, ring.at[way, j, step - 1], rg_send.at[way, j, step - 1], rg_recv.at[way, j, step - 1], dev)

    rcopies = {}

    def combine(j):
        exch[j].wait_recv()
        own = ebuf[j, par].reshape(rows_q, cw)
        other = esib[j].reshape(rows_q, cw)
        for start, width in wide_tiles(cw, 256):
            total = dot32(cmat[0, 0], own[:, start:start + width]) + dot32(cmat[1, 0], other[:, start:start + width])
            for i in (1, 2):
                total += dot32(cmat[0, i], own[:, start:start + width]) + dot32(cmat[1, i], other[:, start:start + width])
            ct[j, :, :, start:start + width] = total.reshape(nz, tok, width)
        for r in range(j * subs, (j + 1) * subs):
            for way in range(2):
                rcopies[way, r, 1] = go(ring_copy(way, r, 1))

    def advance(j, step):
        for way in range(2):
            if step < reach(way, j):
                rcopies[way, j, step].wait_recv()
                ahead = reach(way, j) - step
                dest = chip(ahead if way == 0 else -ahead)
                ring[way, j, step - 1] += ct[j // subs, dest, :, j % subs * rw:(j % subs + 1) * rw]
                rcopies[way, j, step + 1] = go(ring_copy(way, j, step + 1))

    def finish(j):
        cols = slice(j * rw, (j + 1) * rw)
        total = resid_ref[:, cols].astype(F32) + sh_out[:, cols] + ct[j // subs, z, :, j % subs * rw:(j % subs + 1) * rw]
        for way in range(2):
            rcopies[way, j, reach(way, j)].wait_recv()
            total += ring[way, j, reach(way, j) - 1]
        out_ref[:, cols] = total.astype(BF16)
        back = pltpu.make_async_copy(out_ref.at[:, pl.ds(j * rw, rw)], out_hbm.at[:, pl.ds(j * rw, rw)], sem_o.at[j])
        back.start()
        return back

    exch = {}

    def down(j):
        for e in range(e_loc):
            b_copy(j * e_loc + e).wait()
        for e in range(e_loc):
            res = dot32(act[e], b_place(j * e_loc + e)[...]).astype(BF16)
            ebuf[j, 0, e] = res[:rows_par]
            ebuf[j, 1, e] = res[rows_par:]
        exch[j] = go(remote(ebuf.at[j, 1 - par], esib.at[j], ex_send.at[j], ex_recv.at[j], sib))
        shared = CHUNKS * e_loc
        if j == 1:
            a_copy(2 * e_loc + 1).start()
            a_copy(2 * e_loc + 2).start()
        elif j == 2:
            a_copy(2 * e_loc + 3).start()
            for pos in range(SLOTS_B):
                b_copy(shared + pos).start()
        elif j == 3:
            for pos in range(SLOTS_B, CHUNKS * halves):
                b_copy(shared + pos).start()

    def shared_up(hf, tile):
        unit = 2 * e_loc + 2 * hf
        start, width = wide_tiles(ff, TILE)[tile]
        if tile == 0:
            a_copy(unit).wait()
            a_copy(unit + 1).wait()
        act_sh[hf, :, start:start + width] = swiglu_tile(h_ref[...], a_slot(unit), a_slot(unit + 1), start, width)

    def shared_down(j):
        total = jnp.zeros((tok, cw), F32)
        for hf in range(halves):
            unit = CHUNKS * e_loc + j * halves + hf
            b_copy(unit).wait()
            total += dot32(act_sh[hf], b_place(unit)[...])
        sh_out[:, j * cw:(j + 1) * cw] = total

    down(0)
    down(1)
    combine(0)
    down(2)
    combine(1)
    down(3)
    combine(2)
    combine(3)
    tiles = len(wide_tiles(ff, TILE))
    pieces = [functools.partial(shared_up, hf, tile) for hf in range(halves) for tile in range(tiles)]
    pieces += [functools.partial(shared_down, j) for j in range(CHUNKS)]
    events = [(j, step) for step in range(1, far) for j in range(RINGS)]
    early = list(sent)
    gone = 0
    for i, event in enumerate(events):
        until = (i + 1) * len(early) // len(events)
        for copy in early[gone:until]:
            copy.wait_send()
        gone = until
        advance(*event)
        for piece in pieces[i * len(pieces) // len(events):(i + 1) * len(pieces) // len(events)]:
            piece()
    backs = [finish(j) for j in range(RINGS)]
    for copy in sent[len(early):]:
        copy.wait_send()
    for back in backs:
        back.wait()


def moe_call(n_ep, h_norm, table, resid, w_sg, w_su, w_sd, w_eg, w_eu, w_ed):
    nz = n_ep // 2
    tok, dim = h_norm.shape
    e_loc, _, ff = w_eg.shape
    n_exp = e_loc * n_ep
    halves = w_sg.shape[1] // ff
    far = nz // 2
    cw = dim // CHUNKS
    rw = dim // RINGS
    rows_par = nz * CAP
    rows_exp = 2 * rows_par
    rows_all = e_loc * rows_exp
    rows_q = e_loc * rows_par
    row = np.arange(rows_all)
    rowpat = np.zeros((rows_all, 8), np.float32)
    rowpat[:, 0] = row // rows_exp
    rowpat[:, 1] = (row % rows_exp) // CAP
    rowpat[:, 2] = row % CAP + 1
    col = np.arange(rows_q)
    colpat = np.zeros((8, rows_q), np.float32)
    colpat[0] = col // rows_par
    colpat[1] = (col % rows_par) // CAP
    colpat[2] = col % CAP + 1
    hbm = pl.BlockSpec(memory_space=pl.ANY)
    dma = pltpu.SemaphoreType.DMA
    return pl.pallas_call(
        functools.partial(moe_kernel, n_ep, n_exp),
        out_shape=jax.ShapeDtypeStruct((tok, dim), BF16),
        in_specs=[hbm] * 11,
        out_specs=hbm,
        scratch_shapes=[
            pltpu.VMEM((n_ep, tok, dim), BF16),
            pltpu.VMEM((n_ep, tok, LANES), F32),
            pltpu.VMEM((e_loc, rows_exp, dim), BF16),
            pltpu.VMEM((e_loc, rows_exp, ff), BF16),
            pltpu.VMEM((halves, tok, ff), BF16),
            pltpu.VMEM((CHUNKS, 2, e_loc, rows_par, cw), BF16),
            pltpu.VMEM((CHUNKS, e_loc, rows_par, cw), BF16),
            pltpu.VMEM((2, 3, nz * tok, rows_q), BF16),
            pltpu.VMEM((CHUNKS, nz, tok, cw), F32),
            pltpu.VMEM((2, RINGS, far, tok, rw), F32),
            pltpu.VMEM((SLOTS_A, dim, ff), BF16),
            pltpu.VMEM((SLOTS_B, ff, cw), BF16),
            pltpu.VMEM((tok, dim), F32),
            dma((2 * (e_loc + halves),)), dma((CHUNKS * (e_loc + halves),)),
            dma((2, far, PARTS)), dma((2, far, PARTS)), dma((nz,)), dma((nz,)),
            dma((2, far)), dma((2, far)), dma((nz,)), dma((nz,)),
            dma((CHUNKS,)), dma((CHUNKS,)),
            dma((2, RINGS, far)), dma((2, RINGS, far)),
            pltpu.VMEM((tok, dim), BF16),
            pltpu.VMEM((tok, LANES), F32),
            pltpu.VMEM((tok, dim), BF16),
            pltpu.VMEM(rowpat.shape, F32),
            pltpu.VMEM(colpat.shape, F32),
            pltpu.VMEM((tok, dim), BF16),
            dma((5,)), dma((RINGS,)),
        ],
        compiler_params=pltpu.CompilerParams(collective_id=0, has_side_effects=True, vmem_limit_bytes=67000000),
        name='moe_ring',
    )(h_norm, table, resid, jnp.asarray(rowpat), jnp.asarray(colpat), w_sg, w_su, w_sd, w_eg, w_eu, w_ed)


def solution(mesh):
    n_ep = mesh.shape['ep']
    row_one = P(('dp', 'ep'))
    row_two = P(('dp', 'ep'), None)
    row_three = P(('dp', 'ep'), None, None)
    rep_one = P(None)
    rep_two = P(None, None)
    rep_three = P(None, None, None)
    exp_spec = P('ep', None, None)

    def local_step(tok_in, lat_cache, rope_cache, tok_pos, expert_ids, attn_gain, w_query, w_kvdown, w_ukey, w_uval, w_out, ffn_gain, w_router, sh_gate, sh_up, sh_down, ex_gate, ex_up, ex_down):
        resid_bf, h_norm, table, lat_out, rope_out = attn_call(tok_in, lat_cache, rope_cache, tok_pos, expert_ids, attn_gain, w_query, w_kvdown, w_ukey, w_uval, w_out, ffn_gain, w_router)
        out_hidden = moe_call(n_ep, h_norm, table, resid_bf, sh_gate, sh_up, sh_down, ex_gate, ex_up, ex_down)
        return out_hidden, lat_out, rope_out

    in_specs = (row_two, row_three, row_three, row_one, row_two, rep_one, rep_two, rep_two, rep_three, rep_three, rep_two, rep_one, rep_two, rep_two, rep_two, rep_two, exp_spec, exp_spec, exp_spec)
    out_specs = (row_two, row_three, row_three)
    return jax.shard_map(local_step, mesh=mesh, in_specs=in_specs, out_specs=out_specs, check_vma=False)
```

```python
import functools

import jax
import jax.numpy as jnp
import numpy as np
from jax import lax
from jax.experimental import pallas as pl
from jax.experimental.pallas import tpu as pltpu
from jax.sharding import PartitionSpec as P

ROUTE_SCALE = 2.827
ROPE_BASE = 10000.0
NORM_EPS = 1e-6
MESH = pl.DeviceIdType.MESH
F32 = jnp.float32
BF16 = jnp.bfloat16
CHUNKS = 4
RINGS = 4
TILE = 256
SLOTS_A = 7
SLOTS_B = 4
CAP = 6
PARTS = 4
LANES = 128
GROUP = 4


def unit_norm(values):
    mean_sq = jnp.mean(jnp.square(values), axis=-1, keepdims=True)
    return values * lax.rsqrt(mean_sq + NORM_EPS)


def dot32(lhs, rhs):
    return jnp.dot(lhs, rhs, preferred_element_type=F32)


def wide_tiles(total, width):
    return [(start, min(width, total - start)) for start in range(0, total, width)]


def attn_kernel(pos_hbm, x_hbm, freq_hbm, ids_hbm, ag_hbm, fg_hbm, wq_ref, wkv_ref, uk_ref, uv_ref, wo_ref, wr_ref, lat_ref, rope_ref,
                res_ref, h_ref, table_ref, lat_out, rope_out,
                wq, wkv, uk, uv, wo, wr, lat, rope, q_lat, q_rope, o_lat, o_heads, score, prob, pos_ref, x_ref, freq_ref, ids_ref, ag_ref, fg_ref, sem_q, sem_w, sem_c, sem_o, sem_i):
    n_heads, nope, rank = uk_ref.shape
    tok, dim = x_ref.shape
    seq, rope_dim = rope_ref.shape[1:]
    half = rope_dim // 2
    head = nope + rope_dim
    n_exp = wr_ref.shape[0]
    blocks = n_heads // GROUP
    q_cols = GROUP * head

    def q_copy(blk):
        return pltpu.make_async_copy(wq_ref.at[:, pl.ds(blk * q_cols, q_cols)], wq.at[blk], sem_q.at[blk])

    kv_copy = pltpu.make_async_copy(wkv_ref, wkv, sem_w.at[0])
    uk_copy = pltpu.make_async_copy(uk_ref, uk, sem_w.at[1])
    uv_copy = pltpu.make_async_copy(uv_ref, uv, sem_w.at[2])
    wo_copies = [pltpu.make_async_copy(wo_ref.at[:, pl.ds(i * dim // 2, dim // 2)], wo.at[i], sem_w.at[3 + i]) for i in range(2)]
    wr_copy = pltpu.make_async_copy(wr_ref, wr, sem_w.at[5])
    lat_copy = pltpu.make_async_copy(lat_ref, lat, sem_c.at[0])
    rope_copy = pltpu.make_async_copy(rope_ref, rope, sem_c.at[1])
    small = [pltpu.make_async_copy(src, dst, sem_i.at[i]) for i, (src, dst) in enumerate((
        (x_hbm, x_ref), (ag_hbm, ag_ref), (pos_hbm, pos_ref), (freq_hbm, freq_ref), (fg_hbm, fg_ref), (ids_hbm, ids_ref)))]
    for copy in small:
        copy.start()
    kv_copy.start()
    q_copy(0).start()
    uk_copy.start()
    q_copy(1).start()
    for copy in small[:4]:
        copy.wait()

    x = x_ref[...].astype(F32)
    x_norm = (unit_norm(x) * ag_ref[...].astype(F32).reshape(1, dim)).astype(BF16)
    tok_row = lax.broadcasted_iota(jnp.int32, (tok, half), 0)
    pos = jnp.zeros((tok, half), jnp.int32)
    for t in range(tok):
        pos = jnp.where(tok_row == t, pos_ref[t], pos)
    angle = pos.astype(F32) * freq_ref[...]
    cos, sin = jnp.cos(angle), jnp.sin(angle)
    across = (((1,), (1,)), ((), ()))

    def rotate(first, second):
        return jnp.concatenate([first * cos - second * sin, second * cos + first * sin], axis=1)

    kv_copy.wait()
    for blk in range(2, blocks):
        q_copy(blk).start()
    kv = lax.dot_general(x_norm, wkv[...], across, preferred_element_type=F32)
    lat_new = unit_norm(kv[:, :rank]).astype(BF16).astype(F32)
    rope_new = rotate(kv[:, rank:rank + half], kv[:, rank + half:]).astype(BF16).astype(F32)

    def spread(ref, n, val):
        for c in range(val.shape[1] // LANES):
            ref[c, pl.ds(n, tok, stride=n_heads), :] = val[:, c * LANES:(c + 1) * LANES]

    queries = []

    def heads(blk):
        q = queries[blk]
        for i in range(GROUP):
            n = blk * GROUP + i
            at = i * head
            spread(q_lat, n, dot32(q[:, at:at + nope], uk[n]).astype(BF16).astype(F32))
            q_r = q[:, at + nope:at + head].astype(F32)
            q_r = rotate(q_r[:, :half], q_r[:, half:]).astype(BF16).astype(F32)
            spread(q_rope, n, jnp.concatenate([q_r, jnp.zeros((tok, LANES - rope_dim), F32)], axis=1))

    uk_copy.wait()
    for blk in range(blocks):
        q_copy(blk).wait()
        if blk == 0:
            lat_copy.start()
            rope_copy.start()
            uv_copy.start()
        elif blk == 1:
            wr_copy.start()
            for copy in wo_copies:
                copy.start()
        queries.append(dot32(x_norm, wq[blk]).astype(BF16))
        if blk > 0:
            heads(blk - 1)
    lat_copy.wait()
    rope_copy.wait()
    heads(blocks - 1)
    rows, keys = GROUP * n_heads, GROUP * seq
    key = lax.broadcasted_iota(jnp.int32, (rows, keys), 1)
    same = (key // seq) == (lax.broadcasted_iota(jnp.int32, (rows, keys), 0) // n_heads)
    key_tok, key_seq = key // seq, lax.rem(key, seq)
    groups = tok // GROUP

    def grouped(g):
        lat_g = lat[g * GROUP:(g + 1) * GROUP].reshape(keys, rank)
        rope_g = rope[g * GROUP:(g + 1) * GROUP].reshape(keys, rope_dim)
        return slice(g * rows, (g + 1) * rows), lat_g, rope_g

    lat_row = lax.broadcasted_iota(jnp.int32, (seq, rank), 0)
    rope_row = lax.broadcasted_iota(jnp.int32, (seq, rope_dim), 0)
    for t in range(tok):
        lat[t] = jnp.where(lat_row == pos_ref[t], lat_new[t:t + 1], lat[t].astype(F32)).astype(BF16)
        rope[t] = jnp.where(rope_row == pos_ref[t], rope_new[t:t + 1], rope[t].astype(F32)).astype(BF16)
    lat_back = pltpu.make_async_copy(lat, lat_out, sem_o.at[0])
    rope_back = pltpu.make_async_copy(rope, rope_out, sem_o.at[1])
    for g in range(groups):
        sl, lat_g, rope_g = grouped(g)
        q_g = jnp.concatenate([q_lat[c, sl] for c in range(rank // LANES)], axis=1).astype(BF16)
        score[g] = (lax.dot_general(q_g, lat_g, across, preferred_element_type=F32)
                    + lax.dot_general(q_rope[0, sl, :rope_dim].astype(BF16), rope_g, across, preferred_element_type=F32))
    for g in range(groups):
        last = jnp.full((rows, keys), pos_ref[g * GROUP], jnp.int32)
        for i in range(1, GROUP):
            last = jnp.where(key_tok == i, pos_ref[g * GROUP + i], last)
        masked = jnp.where(same & (key_seq <= last), score[g] * head ** -0.5, -jnp.inf)
        expd = jnp.exp(masked - jnp.max(masked, axis=1, keepdims=True))
        prob[g] = (expd / jnp.sum(expd, axis=1, keepdims=True)).astype(BF16)
    for g in range(groups):
        sl, lat_g, _ = grouped(g)
        o_g = dot32(prob[g], lat_g).astype(BF16).astype(F32)
        for c in range(rank // LANES):
            o_lat[c, sl] = o_g[:, c * LANES:(c + 1) * LANES]
    lat_back.start()
    rope_back.start()

    uv_copy.wait()
    for n in range(n_heads):
        o_n = jnp.concatenate([o_lat[c, pl.ds(n, tok, stride=n_heads), :] for c in range(rank // LANES)], axis=1).astype(BF16)
        o_heads[:, n * uv.shape[2]:(n + 1) * uv.shape[2]] = dot32(o_n, uv[n]).astype(BF16)
    for i, copy in enumerate(wo_copies):
        copy.wait()
        for start, width in wide_tiles(dim // 2, 512):
            cols = slice(i * dim // 2 + start, i * dim // 2 + start + width)
            res_ref[:, cols] = (x[:, cols] + dot32(o_heads[...], wo[i, :, start:start + width])).astype(BF16)
    wr_copy.wait()
    for copy in small[4:]:
        copy.wait()
    h = (unit_norm(res_ref[...].astype(F32)) * fg_ref[...].astype(F32).reshape(1, dim)).astype(BF16)
    h_ref[...] = h

    gate = jax.nn.sigmoid(lax.dot_general(h, wr[...], across, preferred_element_type=F32))
    exp_row = lax.broadcasted_iota(jnp.int32, (n_exp, tok), 0)
    listed_t = jnp.zeros((n_exp, tok), F32)
    for i in range(ids_ref.shape[0]):
        listed_t = listed_t + jnp.where(exp_row == ids_ref[i:i + 1, :], 1.0, 0.0)
    listed_t = listed_t.astype(BF16)
    row, col = lax.broadcasted_iota(jnp.int32, (tok, tok), 0), lax.broadcasted_iota(jnp.int32, (tok, tok), 1)
    listed = lax.dot_general(jnp.where(row == col, 1.0, 0.0).astype(BF16), listed_t, across, preferred_element_type=F32)
    slots = lax.dot_general(jnp.where(row >= col, 1.0, 0.0).astype(BF16), listed_t, across, preferred_element_type=F32) * listed
    chosen = gate * listed
    table_ref[:, :n_exp] = ROUTE_SCALE * chosen / jnp.sum(chosen, axis=1, keepdims=True)
    table_ref[:, n_exp:] = slots
    lat_back.wait()
    rope_back.wait()


def attn_call(tok_in, lat_cache, rope_cache, tok_pos, expert_ids, attn_gain, w_query, w_kvdown, w_ukey, w_uval, w_out, ffn_gain, w_router):
    tok, dim = tok_in.shape
    n_heads, nope, rank = w_ukey.shape
    seq, rope_dim = rope_cache.shape[1:]
    n_exp = w_router.shape[1]
    blocks = n_heads // GROUP
    inv_freq = ROPE_BASE ** (-(2.0 * np.arange(rope_dim // 2)) / rope_dim)
    freq = jnp.asarray(inv_freq[None, :].astype(np.float32))
    vmem = pl.BlockSpec(memory_space=pltpu.VMEM)
    hbm = pl.BlockSpec(memory_space=pl.ANY)
    dma = pltpu.SemaphoreType.DMA
    return pl.pallas_call(
        attn_kernel,
        out_shape=[
            jax.ShapeDtypeStruct((tok, dim), BF16),
            jax.ShapeDtypeStruct((tok, dim), BF16),
            jax.ShapeDtypeStruct((tok, 2 * n_exp), F32),
            jax.ShapeDtypeStruct(lat_cache.shape, BF16),
            jax.ShapeDtypeStruct(rope_cache.shape, BF16),
        ],
        in_specs=[hbm] * 14,
        out_specs=[vmem, vmem, vmem, hbm, hbm],
        scratch_shapes=[
            pltpu.VMEM((blocks, dim, w_query.shape[1] // blocks), BF16),
            pltpu.VMEM(w_kvdown.shape[::-1], BF16),
            pltpu.VMEM(w_ukey.shape, BF16),
            pltpu.VMEM(w_uval.shape, BF16),
            pltpu.VMEM((2, w_out.shape[0], dim // 2), BF16),
            pltpu.VMEM(w_router.shape[::-1], BF16),
            pltpu.VMEM(lat_cache.shape, BF16),
            pltpu.VMEM(rope_cache.shape, BF16),
            pltpu.VMEM((rank // LANES, tok * n_heads, LANES), F32),
            pltpu.VMEM((1, tok * n_heads, LANES), F32),
            pltpu.VMEM((rank // LANES, tok * n_heads, LANES), F32),
            pltpu.VMEM((tok, w_out.shape[0]), BF16),
            pltpu.VMEM((tok // GROUP, GROUP * n_heads, GROUP * seq), F32),
            pltpu.VMEM((tok // GROUP, GROUP * n_heads, GROUP * seq), BF16),
            pltpu.SMEM(tok_pos.shape, jnp.int32),
            pltpu.VMEM((tok, dim), BF16),
            pltpu.VMEM(freq.shape, F32),
            pltpu.VMEM(expert_ids.shape[::-1], jnp.int32),
            pltpu.VMEM((dim,), BF16),
            pltpu.VMEM((dim,), BF16),
            dma((blocks,)), dma((6,)), dma((2,)), dma((2,)), dma((6,)),
        ],
        compiler_params=pltpu.CompilerParams(vmem_limit_bytes=60000000),
        name='latent_attention',
    )(tok_pos, tok_in, freq, expert_ids.T, attn_gain, ffn_gain, w_query, w_kvdown.T, w_ukey, w_uval, w_out, w_router.T, lat_cache, rope_cache)


def moe_kernel(n_ep, n_exp, h_hbm, table_hbm, resid_hbm, rowpat_hbm, colpat_hbm,
               sg_ref, su_ref, sd_ref, eg_ref, eu_ref, ed_ref, out_hbm,
               hall, gall, xg, act, act_sh, ebuf, esib, cmat, ct, ring, wa, wb, sh_out,
               sem_a, sem_b, ag_send, ag_recv, sib_send, sib_recv, tb_send, tb_recv, ts_send, ts_recv,
               ex_send, ex_recv, rg_send, rg_recv, h_ref, table_ref, resid_ref, rowpat_ref, colpat_ref, out_ref, sem_i, sem_o):
    nz = n_ep // 2
    far = nz // 2
    tok, dim = h_hbm.shape
    e_loc, _, ff = eg_ref.shape
    halves = sg_ref.shape[1] // ff
    rows_par = nz * CAP
    rows_exp = 2 * rows_par
    rows_all = e_loc * rows_exp
    rows_q = e_loc * rows_par
    cw = dim // CHUNKS
    rw = dim // RINGS
    subs = RINGS // CHUNKS
    part_dim = dim // PARTS

    me = lax.axis_index('ep')
    z = me // 2
    par = lax.rem(me, 2)
    sib = me + 1 - 2 * par
    up_dev = lax.rem(z + 1, nz) * 2 + par
    dn_dev = lax.rem(z + nz - 1, nz) * 2 + par

    def chip(step):
        return lax.rem(z + step + 2 * nz, nz)

    def slot_of(p, zz):
        return p * nz + zz

    def a_slot(unit):
        return unit % SLOTS_A if unit < 2 * e_loc else unit - 2 * e_loc

    def a_copy(unit):
        slot = a_slot(unit)
        if unit < 2 * e_loc:
            src = (eg_ref if unit % 2 == 0 else eu_ref).at[unit // 2]
        else:
            hf = (unit - 2 * e_loc) // 2
            src = (sg_ref if unit % 2 == 0 else su_ref).at[:, pl.ds(hf * ff, ff)]
        return pltpu.make_async_copy(src, wa.at[slot], sem_a.at[unit])

    def b_place(unit):
        if unit >= CHUNKS * e_loc + SLOTS_B:
            pos = unit - CHUNKS * e_loc - SLOTS_B
            slot, side = 5 + pos // 2, pos % 2
        elif unit >= CHUNKS * e_loc:
            return wb.at[unit - CHUNKS * e_loc]
        elif unit >= SLOTS_B:
            slot, side = 1 + (unit - SLOTS_B) // 2, unit % 2
        else:
            return wb.at[unit]
        return wa.at[slot, pl.ds(0, ff), pl.ds(side * cw, cw)]

    def b_copy(unit):
        if unit < CHUNKS * e_loc:
            j, e = unit // e_loc, unit % e_loc
            src = ed_ref.at[e, :, pl.ds(j * cw, cw)]
        else:
            j, hf = (unit - CHUNKS * e_loc) // halves, (unit - CHUNKS * e_loc) % halves
            src = sd_ref.at[pl.ds(hf * ff, ff), pl.ds(j * cw, cw)]
        return pltpu.make_async_copy(src, b_place(unit), sem_b.at[unit])

    small = [pltpu.make_async_copy(src, dst, sem_i.at[i]) for i, (src, dst) in enumerate((
        (table_hbm, table_ref), (h_hbm, h_ref), (resid_hbm, resid_ref), (rowpat_hbm, rowpat_ref), (colpat_hbm, colpat_ref)))]
    for copy in small:
        copy.start()

    barrier = pltpu.get_barrier_semaphore()
    for dev in (up_dev, dn_dev, sib):
        pl.semaphore_signal(barrier, inc=1, device_id={'ep': dev}, device_id_type=MESH)
    for unit in range(SLOTS_A):
        a_copy(unit).start()
    for unit in range(SLOTS_B):
        b_copy(unit).start()
    for copy in small:
        copy.wait()
    pl.semaphore_wait(barrier, 3)

    def remote(src, dst, send, recv, dev):
        return pltpu.make_async_remote_copy(src_ref=src, dst_ref=dst, send_sem=send, recv_sem=recv,
                                            device_id={'ep': dev}, device_id_type=MESH)

    def h_hop(way, step, part):
        dev = up_dev if way == 0 else dn_dev
        origin = chip(-step if way == 0 else step)
        slot = slot_of(par, origin)
        cols = pl.ds(part * part_dim, part_dim)
        src = h_ref.at[:, cols] if step == 0 else hall.at[slot, :, cols]
        return remote(src, hall.at[slot, :, cols], ag_send.at[way, step, part], ag_recv.at[way, step, part], dev)

    def t_hop(way, step):
        dev = up_dev if way == 0 else dn_dev
        origin = chip(-step if way == 0 else step)
        slot = slot_of(par, origin)
        src = table_ref if step == 0 else gall.at[slot]
        return remote(src, gall.at[slot], tb_send.at[way, step], tb_recv.at[way, step], dev)

    def h_cross(k, origin):
        slot = slot_of(par, origin)
        src = h_ref if k == 0 else hall.at[slot]
        return remote(src, hall.at[slot], sib_send.at[k], sib_recv.at[k], sib)

    def t_cross(k, origin):
        slot = slot_of(par, origin)
        src = table_ref if k == 0 else gall.at[slot]
        return remote(src, gall.at[slot], ts_send.at[k], ts_recv.at[k], sib)

    t_steps = (far, far - 1)

    def place_rows():
        rowpat = rowpat_ref[...]
        row_exp, row_dev, row_slot = rowpat[:, 0:1], rowpat[:, 1:2], rowpat[:, 2:3]
        base = n_exp + e_loc * me
        lane = lax.broadcasted_iota(jnp.int32, (rows_all, LANES), 1)
        pick = jnp.where(lane == base + row_exp.astype(jnp.int32), 1.0, 0.0).astype(BF16)
        slots_by_row = lax.dot_general(pick, gall[...].reshape(n_ep * tok, LANES).astype(BF16), (((1,), (1,)), ((), ())),
                                       preferred_element_type=F32)
        tok_dev = (lax.broadcasted_iota(jnp.int32, (rows_all, n_ep * tok), 1) // tok).astype(F32)
        return jnp.where((slots_by_row == row_slot) & (tok_dev == row_dev), 1.0, 0.0).astype(BF16)

    def combine_weights():
        colpat = colpat_ref[...]
        col_exp, col_chip, col_slot = colpat[0:1, :], colpat[1:2, :], colpat[2:3, :]
        g_own = gall[pl.ds(par * nz, nz)].reshape(nz * tok, LANES)
        part1 = g_own.astype(BF16)
        rest1 = g_own - part1.astype(F32)
        part2 = rest1.astype(BF16)
        part3 = (rest1 - part2.astype(F32)).astype(BF16)
        sub = lax.broadcasted_iota(jnp.int32, (LANES, rows_q), 0)
        tok_chip = (lax.broadcasted_iota(jnp.int32, (nz * tok, rows_q), 0) // tok).astype(F32)
        for q in range(2):
            ids = e_loc * (me if q == 0 else sib) + col_exp.astype(jnp.int32)
            sel_w = jnp.where(sub == ids, 1.0, 0.0).astype(BF16)
            sel_s = jnp.where(sub == n_exp + ids, 1.0, 0.0).astype(BF16)
            here = (dot32(part1, sel_s) == col_slot) & (tok_chip == col_chip)
            for i, part in enumerate((part1, part2, part3)):
                cmat[q, i] = jnp.where(here, dot32(part, sel_w), 0.0).astype(BF16)
    sent = []

    def go(copy):
        copy.start()
        sent.append(copy)
        return copy

    hops, thops = {}, {}

    def goes(way, step, part):
        return step < far - 1 or part // (PARTS // 2) == way

    for way in range(2):
        thops[way, 0] = go(t_hop(way, 0))
    for part in range(PARTS):
        for way in range(2):
            hops[way, 0, part] = go(h_hop(way, 0, part))
    t_crossed, h_crossed = [go(t_cross(0, z))], [go(h_cross(0, z))]
    hall[slot_of(par, z)] = h_ref[...]
    gall[slot_of(par, z)] = table_ref[...]
    for step in range(far):
        for way in range(2):
            if step < t_steps[way]:
                origin = chip(-(step + 1) if way == 0 else step + 1)
                thops[way, step].wait_recv()
                if step + 1 < t_steps[way]:
                    thops[way, step + 1] = go(t_hop(way, step + 1))
                t_crossed.append(go(t_cross(1 + 2 * step + way, origin)))
        if step == far - 1:
            for copy in t_crossed:
                copy.wait_recv()
            place = place_rows()
            combine_weights()
        for part in range(PARTS):
            for way in range(2):
                if goes(way, step, part):
                    hops[way, step, part].wait_recv()
                    if step + 1 < far and goes(way, step + 1, part):
                        hops[way, step + 1, part] = go(h_hop(way, step + 1, part))
        if step < far - 1:
            for way in range(2):
                h_crossed.append(go(h_cross(1 + 2 * step + way, chip(-(step + 1) if way == 0 else step + 1))))
    h_crossed.append(go(h_cross(2 * far - 1, chip(far))))
    for copy in h_crossed:
        copy.wait_recv()
    for start, width in wide_tiles(dim, 256):
        rows = hall[:, :, start:start + width].reshape(n_ep * tok, width)
        xg[:, :, start:start + width] = dot32(place, rows).astype(BF16).reshape(e_loc, rows_exp, width)

    def swiglu_tile(x, slot_g, slot_u, start, width):
        gate = dot32(x, wa[slot_g, :, start:start + width])
        up = dot32(x, wa[slot_u, :, start:start + width])
        return (jax.nn.silu(gate) * up).astype(BF16)

    def expert_up(e, carry):
        slot_g = lax.rem(2 * e, SLOTS_A)
        slot_u = lax.rem(2 * e + 1, SLOTS_A)
        for unit, slot in ((2 * e, slot_g), (2 * e + 1, slot_u)):
            pltpu.make_async_copy(eg_ref.at[0], wa.at[slot], sem_a.at[unit]).wait()
        for start, width in wide_tiles(ff, TILE):
            act[e, :, start:start + width] = swiglu_tile(xg[e], slot_g, slot_u, start, width)
        for e_st in range(e_loc):
            @pl.when(e == e_st)
            def _():
                if e_st == 0:
                    a_copy(SLOTS_A).start()
                    ahead = (4, 5)
                elif e_st < e_loc - 1:
                    ahead = range(4 * e_st + 2, 4 * e_st + 6)
                else:
                    ahead = (14, 15)
                for unit in ahead:
                    b_copy(unit).start()
                if e_st == e_loc - 1:
                    a_copy(2 * e_loc).start()
        return carry

    lax.fori_loop(0, e_loc, expert_up, 0)

    def reach(way, j):
        return far if (way + j) % 2 == 0 else nz - 1 - far

    def ring_copy(way, j, step):
        dev = up_dev if way == 0 else dn_dev
        ahead = reach(way, j) - step + 1
        dest = chip(ahead if way == 0 else -ahead)
        src = ct.at[j // subs, dest, :, pl.ds(j % subs * rw, rw)] if step == 1 else ring.at[way, j, step - 2]
        return remote(src, ring.at[way, j, step - 1], rg_send.at[way, j, step - 1], rg_recv.at[way, j, step - 1], dev)

    rcopies = {}

    def combine(j):
        exch[j].wait_recv()
        own = ebuf[j, par].reshape(rows_q, cw)
        other = esib[j].reshape(rows_q, cw)
        for start, width in wide_tiles(cw, 256):
            total = dot32(cmat[0, 0], own[:, start:start + width]) + dot32(cmat[1, 0], other[:, start:start + width])
            for i in (1, 2):
                total += dot32(cmat[0, i], own[:, start:start + width]) + dot32(cmat[1, i], other[:, start:start + width])
            ct[j, :, :, start:start + width] = total.reshape(nz, tok, width)
        for r in range(j * subs, (j + 1) * subs):
            for way in range(2):
                rcopies[way, r, 1] = go(ring_copy(way, r, 1))

    def advance(j, step):
        for way in range(2):
            if step < reach(way, j):
                rcopies[way, j, step].wait_recv()
                ahead = reach(way, j) - step
                dest = chip(ahead if way == 0 else -ahead)
                ring[way, j, step - 1] += ct[j // subs, dest, :, j % subs * rw:(j % subs + 1) * rw]
                rcopies[way, j, step + 1] = go(ring_copy(way, j, step + 1))

    def finish(j):
        cols = slice(j * rw, (j + 1) * rw)
        total = resid_ref[:, cols].astype(F32) + sh_out[:, cols] + ct[j // subs, z, :, j % subs * rw:(j % subs + 1) * rw]
        for way in range(2):
            rcopies[way, j, reach(way, j)].wait_recv()
            total += ring[way, j, reach(way, j) - 1]
        out_ref[:, cols] = total.astype(BF16)
        back = pltpu.make_async_copy(out_ref.at[:, pl.ds(j * rw, rw)], out_hbm.at[:, pl.ds(j * rw, rw)], sem_o.at[j])
        back.start()
        return back

    exch = {}

    def down(j):
        for e in range(e_loc):
            b_copy(j * e_loc + e).wait()
        for e in range(e_loc):
            res = dot32(act[e], b_place(j * e_loc + e)[...]).astype(BF16)
            ebuf[j, 0, e] = res[:rows_par]
            ebuf[j, 1, e] = res[rows_par:]
        exch[j] = go(remote(ebuf.at[j, 1 - par], esib.at[j], ex_send.at[j], ex_recv.at[j], sib))
        shared = CHUNKS * e_loc
        if j == 1:
            a_copy(2 * e_loc + 1).start()
            a_copy(2 * e_loc + 2).start()
        elif j == 2:
            a_copy(2 * e_loc + 3).start()
            for pos in range(SLOTS_B):
                b_copy(shared + pos).start()
        elif j == 3:
            for pos in range(SLOTS_B, CHUNKS * halves):
                b_copy(shared + pos).start()

    def shared_up(hf, tile):
        unit = 2 * e_loc + 2 * hf
        start, width = wide_tiles(ff, TILE)[tile]
        if tile == 0:
            a_copy(unit).wait()
            a_copy(unit + 1).wait()
        act_sh[hf, :, start:start + width] = swiglu_tile(h_ref[...], a_slot(unit), a_slot(unit + 1), start, width)

    def shared_down(j):
        total = jnp.zeros((tok, cw), F32)
        for hf in range(halves):
            unit = CHUNKS * e_loc + j * halves + hf
            b_copy(unit).wait()
            total += dot32(act_sh[hf], b_place(unit)[...])
        sh_out[:, j * cw:(j + 1) * cw] = total

    down(0)
    down(1)
    combine(0)
    down(2)
    combine(1)
    down(3)
    combine(2)
    combine(3)
    tiles = len(wide_tiles(ff, TILE))
    pieces = [functools.partial(shared_up, hf, tile) for hf in range(halves) for tile in range(tiles)]
    pieces += [functools.partial(shared_down, j) for j in range(CHUNKS)]
    events = [(j, step) for step in range(1, far) for j in range(RINGS)]
    early = list(sent)
    gone = 0
    for i, event in enumerate(events):
        until = (i + 1) * len(early) // len(events)
        for copy in early[gone:until]:
            copy.wait_send()
        gone = until
        advance(*event)
        for piece in pieces[i * len(pieces) // len(events):(i + 1) * len(pieces) // len(events)]:
            piece()
    backs = [finish(j) for j in range(RINGS)]
    for copy in sent[len(early):]:
        copy.wait_send()
    for back in backs:
        back.wait()


def moe_call(n_ep, h_norm, table, resid, w_sg, w_su, w_sd, w_eg, w_eu, w_ed):
    nz = n_ep // 2
    tok, dim = h_norm.shape
    e_loc, _, ff = w_eg.shape
    n_exp = e_loc * n_ep
    halves = w_sg.shape[1] // ff
    far = nz // 2
    cw = dim // CHUNKS
    rw = dim // RINGS
    rows_par = nz * CAP
    rows_exp = 2 * rows_par
    rows_all = e_loc * rows_exp
    rows_q = e_loc * rows_par
    row = np.arange(rows_all)
    rowpat = np.zeros((rows_all, 8), np.float32)
    rowpat[:, 0] = row // rows_exp
    rowpat[:, 1] = (row % rows_exp) // CAP
    rowpat[:, 2] = row % CAP + 1
    col = np.arange(rows_q)
    colpat = np.zeros((8, rows_q), np.float32)
    colpat[0] = col // rows_par
    colpat[1] = (col % rows_par) // CAP
    colpat[2] = col % CAP + 1
    hbm = pl.BlockSpec(memory_space=pl.ANY)
    dma = pltpu.SemaphoreType.DMA
    return pl.pallas_call(
        functools.partial(moe_kernel, n_ep, n_exp),
        out_shape=jax.ShapeDtypeStruct((tok, dim), BF16),
        in_specs=[hbm] * 11,
        out_specs=hbm,
        scratch_shapes=[
            pltpu.VMEM((n_ep, tok, dim), BF16),
            pltpu.VMEM((n_ep, tok, LANES), F32),
            pltpu.VMEM((e_loc, rows_exp, dim), BF16),
            pltpu.VMEM((e_loc, rows_exp, ff), BF16),
            pltpu.VMEM((halves, tok, ff), BF16),
            pltpu.VMEM((CHUNKS, 2, e_loc, rows_par, cw), BF16),
            pltpu.VMEM((CHUNKS, e_loc, rows_par, cw), BF16),
            pltpu.VMEM((2, 3, nz * tok, rows_q), BF16),
            pltpu.VMEM((CHUNKS, nz, tok, cw), F32),
            pltpu.VMEM((2, RINGS, far, tok, rw), F32),
            pltpu.VMEM((SLOTS_A, dim, ff), BF16),
            pltpu.VMEM((SLOTS_B, ff, cw), BF16),
            pltpu.VMEM((tok, dim), F32),
            dma((2 * (e_loc + halves),)), dma((CHUNKS * (e_loc + halves),)),
            dma((2, far, PARTS)), dma((2, far, PARTS)), dma((nz,)), dma((nz,)),
            dma((2, far)), dma((2, far)), dma((nz,)), dma((nz,)),
            dma((CHUNKS,)), dma((CHUNKS,)),
            dma((2, RINGS, far)), dma((2, RINGS, far)),
            pltpu.VMEM((tok, dim), BF16),
            pltpu.VMEM((tok, LANES), F32),
            pltpu.VMEM((tok, dim), BF16),
            pltpu.VMEM(rowpat.shape, F32),
            pltpu.VMEM(colpat.shape, F32),
            pltpu.VMEM((tok, dim), BF16),
            dma((5,)), dma((RINGS,)),
        ],
        compiler_params=pltpu.CompilerParams(collective_id=0, has_side_effects=True, vmem_limit_bytes=67000000),
        name='moe_ring',
    )(h_norm, table, resid, jnp.asarray(rowpat), jnp.asarray(colpat), w_sg, w_su, w_sd, w_eg, w_eu, w_ed)


def solution(mesh):
    n_ep = mesh.shape['ep']
    row_one = P(('dp', 'ep'))
    row_two = P(('dp', 'ep'), None)
    row_three = P(('dp', 'ep'), None, None)
    rep_one = P(None)
    rep_two = P(None, None)
    rep_three = P(None, None, None)
    exp_spec = P('ep', None, None)

    def local_step(tok_in, lat_cache, rope_cache, tok_pos, expert_ids, attn_gain, w_query, w_kvdown, w_ukey, w_uval, w_out, ffn_gain, w_router, sh_gate, sh_up, sh_down, ex_gate, ex_up, ex_down):
        resid_bf, h_norm, table, lat_out, rope_out = attn_call(tok_in, lat_cache, rope_cache, tok_pos, expert_ids, attn_gain, w_query, w_kvdown, w_ukey, w_uval, w_out, ffn_gain, w_router)
        out_hidden = moe_call(n_ep, h_norm, table, resid_bf, sh_gate, sh_up, sh_down, ex_gate, ex_up, ex_down)
        return out_hidden, lat_out, rope_out

    in_specs = (row_two, row_three, row_three, row_one, row_two, rep_one, rep_two, rep_two, rep_three, rep_three, rep_two, rep_one, rep_two, rep_two, rep_two, rep_two, exp_spec, exp_spec, exp_spec)
    out_specs = (row_two, row_three, row_three)
    return jax.shard_map(local_step, mesh=mesh, in_specs=in_specs, out_specs=out_specs, check_vma=False)
```
